32 devices in a mesh: dp: 4 (over z), tp: 8 (over y, x, core).
Axes of the slice: x: 2, y: 2, z: 4, core: 2. Of those that a mesh axis runs over, the one named last changes fastest.
Arguments:
- hidden: bfloat16 [24, 128, 3584], P('dp', 'tp'), parts along dimension 0
- vision: bfloat16 [24, 2048, 3584], P('dp', 'tp'), parts along dimension 0
- positions: int32 [24, 128], P('dp', 'tp'), parts along dimension 0
- tile_mask: int32 [24, 128, 4], P('dp', 'tp'), parts along dimension 0
- ln1_a: bfloat16 [3584], replicated
- wq_a: bfloat16 [3584, 4096], P(None, 'tp')
- wk_a: bfloat16 [3584, 2048], P(None, 'tp')
- wv_a: bfloat16 [3584, 2048], P(None, 'tp')
- wo_a: bfloat16 [4096, 3584], P('tp')
- ln2_a: bfloat16 [3584], replicated
- wg_a: bfloat16 [3584, 14336], P(None, 'tp')
- wu_a: bfloat16 [3584, 14336], P(None, 'tp')
- wd_a: bfloat16 [14336, 3584], P('tp')
- ln1_b: bfloat16 [3584], replicated
- wq_b: bfloat16 [3584, 4096], P(None, 'tp')
- q_norm: bfloat16 [256], replicated
- wk_b: bfloat16 [3584, 2048], P(None, 'tp')
- wv_b: bfloat16 [3584, 2048], P(None, 'tp')
- k_norm: bfloat16 [256], replicated
- wo_b: bfloat16 [4096, 3584], P('tp')
- ln2_b: bfloat16 [3584], replicated
- wg_b: bfloat16 [3584, 14336], P(None, 'tp')
- wu_b: bfloat16 [3584, 14336], P(None, 'tp')
- wd_b: bfloat16 [14336, 3584], P('tp')
- xgates: float32 [2], replicated
Outputs:
- output: bfloat16 [24, 128, 3584], P('dp', 'tp'), parts along dimension 0
There are 4 independent parts. The reference program is written for one: setup_inputs(seed, part) draws one part's arguments, and reference() takes and returns one part's arrays. A program takes and returns all parts, laid end to end along the dimension named above; an argument that names none is the same for every part.
All inputs are finite; a program needn't handle non-finite values.
Results may differ from the reference program's by a relative error of at most 0.0163982.
Values are sent between devices in bfloat16 or wider.
A program may use at most 1 GiB of HBM per device.

```python
import math
import jax
import jax.numpy as jnp
from jax import lax

SAMPLES = 6
TOKENS = 128
VISION_TOKENS = 2048
MODEL_DIM = 3584
NUM_HEADS = 16
KV_HEADS = 8
HEAD_DIM = 256
FFN_DIM = 14336
NUM_TILES = 4

ROPE_THETA = 500000.0
ROPE_FACTOR = 8.0
LOW_FACTOR = 1.0
HIGH_FACTOR = 4.0
ORIG_CONTEXT = 8192.0
NORM_EPS = 1e-5
MASK_VALUE = -1e30


def rope_table(head_dim):
    low_wave = ORIG_CONTEXT / LOW_FACTOR
    high_wave = ORIG_CONTEXT / HIGH_FACTOR
    freq_list = []
    for freq_idx in range(head_dim // 2):
        base_freq = 1.0 / (ROPE_THETA ** (2.0 * freq_idx / head_dim))
        wave_len = 2.0 * math.pi / base_freq
        if wave_len > low_wave:
            freq_list.append(base_freq / ROPE_FACTOR)
        elif wave_len < high_wave:
            freq_list.append(base_freq)
        else:
            smooth = (ORIG_CONTEXT / wave_len - LOW_FACTOR) / (HIGH_FACTOR - LOW_FACTOR)
            freq_list.append((1.0 - smooth) * base_freq / ROPE_FACTOR + smooth * base_freq)
    return jnp.array(freq_list, dtype=jnp.float32)


def rms_scale(values, norm_gain):
    values = values.astype(jnp.float32)
    mean_sq = jnp.mean(values * values, axis=-1, keepdims=True)
    return values * lax.rsqrt(mean_sq + NORM_EPS) * norm_gain.astype(jnp.float32)


def rotate(values, cos_tab, sin_tab):
    half_dim = values.shape[-1] // 2
    first_half = values[..., :half_dim]
    second_half = values[..., half_dim:]
    return jnp.concatenate([first_half * cos_tab - second_half * sin_tab, second_half * cos_tab + first_half * sin_tab], axis=-1)


def group_attention(queries, key_vecs, val_vecs, allowed):
    def one_group(operands):
        query_grp, key_grp, val_grp = operands
        scores = jnp.einsum('rqd,kd->rqk', query_grp.astype(jnp.float32), key_grp.astype(jnp.float32)) * (HEAD_DIM ** -0.5)
        weights = jax.nn.softmax(jnp.where(allowed[None], scores, MASK_VALUE), axis=-1).astype(jnp.bfloat16)
        return jnp.einsum('rqk,kd->rqd', weights.astype(jnp.float32), val_grp.astype(jnp.float32)).astype(jnp.bfloat16)
    grouped = lax.map(one_group, (jnp.transpose(queries, (1, 2, 0, 3)), jnp.transpose(key_vecs, (1, 0, 2)), jnp.transpose(val_vecs, (1, 0, 2))))
    return jnp.transpose(grouped, (2, 0, 1, 3)).reshape(queries.shape[0], -1)


def gated_mlp(resid, norm_gain, w_gate, w_up, w_down):
    normed = rms_scale(resid, norm_gain).astype(jnp.bfloat16)
    gate_proj = jnp.dot(normed, w_gate, preferred_element_type=jnp.float32)
    up_proj = jnp.dot(normed, w_up, preferred_element_type=jnp.float32)
    activated = (jax.nn.silu(gate_proj) * up_proj).astype(jnp.bfloat16)
    return jnp.dot(activated, w_down, preferred_element_type=jnp.float32)


def setup_inputs(seed: int = 0, part: int = 0) -> dict:
    data_keys = jax.random.split(jax.random.fold_in(jax.random.key(seed + 1), part), 6)
    weight_keys = jax.random.split(jax.random.key(seed), 22)
    qk_scale = max(math.log(TOKENS / 8.0), 1.0) ** 0.25
    cross_gain = max(math.log(VISION_TOKENS / 16.0), 1.0) ** 0.25
    q_width = NUM_HEADS * HEAD_DIM
    kv_width = KV_HEADS * HEAD_DIM
    dim_scale = MODEL_DIM ** -0.5

    def draw_normal(key_val, arr_shape, spread):
        return (jax.random.normal(key_val, arr_shape, jnp.float32) * spread).astype(jnp.bfloat16)

    def draw_gain(key_val, arr_shape, center):
        return (center * (1.0 + 0.2 * jax.random.normal(key_val, arr_shape, jnp.float32))).astype(jnp.bfloat16)

    hidden = draw_normal(data_keys[0], (SAMPLES, TOKENS, MODEL_DIM), 1.0)
    vision = draw_normal(data_keys[1], (SAMPLES, VISION_TOKENS, MODEL_DIM), 1.0)
    pos_steps = jax.random.randint(data_keys[2], (SAMPLES, TOKENS), 1, 4, dtype=jnp.int32)
    offsets = jax.random.randint(data_keys[3], (SAMPLES, 1), 0, TOKENS, dtype=jnp.int32)
    positions = (offsets + jnp.cumsum(pos_steps, axis=1)).astype(jnp.int32)
    begins = jax.random.randint(data_keys[4], (SAMPLES, 1, 1), 0, TOKENS // 4 + 1, dtype=jnp.int32)
    tile_bits = jax.random.randint(data_keys[5], (SAMPLES, TOKENS, NUM_TILES), 0, 2, dtype=jnp.int32)
    tile_mask = jnp.where(jnp.arange(TOKENS, dtype=jnp.int32)[None, :, None] >= begins, tile_bits, 0).astype(jnp.int32)
    magnitudes = jax.random.uniform(weight_keys[20], (2,), jnp.float32, 0.6, 1.4)
    gate_signs = (2 * jax.random.randint(weight_keys[21], (2,), 0, 2, dtype=jnp.int32) - 1).astype(jnp.float32)
    return {
        'hidden': hidden,
        'vision': vision,
        'positions': positions,
        'tile_mask': tile_mask,
        'ln1_a': draw_gain(weight_keys[0], (MODEL_DIM,), 1.0),
        'wq_a': draw_normal(weight_keys[1], (MODEL_DIM, q_width), qk_scale * dim_scale),
        'wk_a': draw_normal(weight_keys[2], (MODEL_DIM, kv_width), qk_scale * dim_scale),
        'wv_a': draw_normal(weight_keys[3], (MODEL_DIM, kv_width), dim_scale),
        'wo_a': draw_normal(weight_keys[4], (q_width, MODEL_DIM), q_width ** -0.5),
        'ln2_a': draw_gain(weight_keys[5], (MODEL_DIM,), 1.0),
        'wg_a': draw_normal(weight_keys[6], (MODEL_DIM, FFN_DIM), dim_scale),
        'wu_a': draw_normal(weight_keys[7], (MODEL_DIM, FFN_DIM), dim_scale),
        'wd_a': draw_normal(weight_keys[8], (FFN_DIM, MODEL_DIM), FFN_DIM ** -0.5),
        'ln1_b': draw_gain(weight_keys[9], (MODEL_DIM,), 1.0),
        'wq_b': draw_normal(weight_keys[10], (MODEL_DIM, q_width), dim_scale),
        'q_norm': draw_gain(weight_keys[11], (HEAD_DIM,), cross_gain),
        'wk_b': draw_normal(weight_keys[12], (MODEL_DIM, kv_width), dim_scale),
        'wv_b': draw_normal(weight_keys[13], (MODEL_DIM, kv_width), dim_scale),
        'k_norm': draw_gain(weight_keys[14], (HEAD_DIM,), cross_gain),
        'wo_b': draw_normal(weight_keys[15], (q_width, MODEL_DIM), q_width ** -0.5),
        'ln2_b': draw_gain(weight_keys[16], (MODEL_DIM,), 1.0),
        'wg_b': draw_normal(weight_keys[17], (MODEL_DIM, FFN_DIM), dim_scale),
        'wu_b': draw_normal(weight_keys[18], (MODEL_DIM, FFN_DIM), dim_scale),
        'wd_b': draw_normal(weight_keys[19], (FFN_DIM, MODEL_DIM), FFN_DIM ** -0.5),
        'xgates': magnitudes * gate_signs,
    }


def reference(hidden, vision, positions, tile_mask, ln1_a, wq_a, wk_a, wv_a, wo_a, ln2_a, wg_a, wu_a, wd_a, ln1_b, wq_b, q_norm, wk_b, wv_b, k_norm, wo_b, ln2_b, wg_b, wu_b, wd_b, xgates):
    rep_heads = NUM_HEADS // KV_HEADS
    tile_len = VISION_TOKENS // NUM_TILES
    inv_freq = rope_table(HEAD_DIM)
    gate_vals = jnp.tanh(xgates.astype(jnp.float32))
    causal = lax.broadcasted_iota(jnp.int32, (TOKENS, TOKENS), 0) >= lax.broadcasted_iota(jnp.int32, (TOKENS, TOKENS), 1)

    def one_sample(operands):
        hid_rows, vis_rows, pos_row, mask_row = operands
        angles = pos_row.astype(jnp.float32)[:, None] * inv_freq[None, :]
        cos_tab = jnp.cos(angles)[:, None, :]
        sin_tab = jnp.sin(angles)[:, None, :]
        normed = rms_scale(hid_rows, ln1_a).astype(jnp.bfloat16)
        queries = jnp.dot(normed, wq_a, preferred_element_type=jnp.float32).reshape(TOKENS, NUM_HEADS, HEAD_DIM)
        queries = rotate(queries, cos_tab, sin_tab).astype(jnp.bfloat16).reshape(TOKENS, KV_HEADS, rep_heads, HEAD_DIM)
        key_vecs = jnp.dot(normed, wk_a, preferred_element_type=jnp.float32).reshape(TOKENS, KV_HEADS, HEAD_DIM)
        key_vecs = rotate(key_vecs, cos_tab, sin_tab).astype(jnp.bfloat16)
        val_vecs = jnp.dot(normed, wv_a, preferred_element_type=jnp.float32).astype(jnp.bfloat16).reshape(TOKENS, KV_HEADS, HEAD_DIM)
        context = group_attention(queries, key_vecs, val_vecs, causal)
        h_one = (hid_rows.astype(jnp.float32) + jnp.dot(context, wo_a, preferred_element_type=jnp.float32)).astype(jnp.bfloat16)
        h_two = (h_one.astype(jnp.float32) + gated_mlp(h_one, ln2_a, wg_a, wu_a, wd_a)).astype(jnp.bfloat16)
        normed = rms_scale(h_two, ln1_b).astype(jnp.bfloat16)
        queries = jnp.dot(normed, wq_b, preferred_element_type=jnp.float32).reshape(TOKENS, NUM_HEADS, HEAD_DIM)
        queries = rms_scale(queries, q_norm).astype(jnp.bfloat16).reshape(TOKENS, KV_HEADS, rep_heads, HEAD_DIM)
        key_vecs = jnp.dot(vis_rows, wk_b, preferred_element_type=jnp.float32).reshape(VISION_TOKENS, KV_HEADS, HEAD_DIM)
        key_vecs = rms_scale(key_vecs, k_norm).astype(jnp.bfloat16)
        val_vecs = jnp.dot(vis_rows, wv_b, preferred_element_type=jnp.float32).astype(jnp.bfloat16).reshape(VISION_TOKENS, KV_HEADS, HEAD_DIM)
        visible = mask_row > 0
        allowed = jnp.repeat(visible, tile_len, axis=1)
        context = group_attention(queries, key_vecs, val_vecs, allowed)
        row_keep = jnp.any(visible, axis=-1, keepdims=True).astype(jnp.float32)
        attn_out = jnp.dot(context, wo_b, preferred_element_type=jnp.float32)
        h_three = (h_two.astype(jnp.float32) + gate_vals[0] * row_keep * attn_out).astype(jnp.bfloat16)
        mlp_out = gated_mlp(h_three, ln2_b, wg_b, wu_b, wd_b)
        return (h_three.astype(jnp.float32) + gate_vals[1] * row_keep * mlp_out).astype(jnp.bfloat16)

    return lax.map(one_sample, (hidden, vision, positions, tile_mask))
```

```python
import functools
import math
import jax
import jax.numpy as jnp
from jax import lax
from jax.experimental import pallas as pl
from jax.experimental.pallas import tpu as pltpu
from jax.sharding import PartitionSpec as P

ROPE_THETA = 500000.0
ROPE_FACTOR = 8.0
LOW_FACTOR = 1.0
HIGH_FACTOR = 4.0
ORIG_CONTEXT = 8192.0
NORM_EPS = 1e-5
MASK_VALUE = -1e30


def rope_table(head_dim):
    low_wave = ORIG_CONTEXT / LOW_FACTOR
    high_wave = ORIG_CONTEXT / HIGH_FACTOR
    freq_list = []
    for freq_idx in range(head_dim // 2):
        base_freq = 1.0 / (ROPE_THETA ** (2.0 * freq_idx / head_dim))
        wave_len = 2.0 * math.pi / base_freq
        if wave_len > low_wave:
            freq_list.append(base_freq / ROPE_FACTOR)
        elif wave_len < high_wave:
            freq_list.append(base_freq)
        else:
            smooth = (ORIG_CONTEXT / wave_len - LOW_FACTOR) / (HIGH_FACTOR - LOW_FACTOR)
            freq_list.append((1.0 - smooth) * base_freq / ROPE_FACTOR + smooth * base_freq)
    return jnp.array(freq_list, dtype=jnp.float32)


def rms_scale(values, norm_gain):
    values = values.astype(jnp.float32)
    mean_sq = jnp.mean(values * values, axis=-1, keepdims=True)
    return values * lax.rsqrt(mean_sq + NORM_EPS) * norm_gain.astype(jnp.float32)


def rotate(values, cos_tab, sin_tab):
    half_dim = values.shape[-1] // 2
    first_half = values[..., :half_dim]
    second_half = values[..., half_dim:]
    return jnp.concatenate([first_half * cos_tab - second_half * sin_tab, second_half * cos_tab + first_half * sin_tab], axis=-1)


def self_attend(queries, key_vecs, val_vecs):
    seq_len = queries.shape[3]
    head_dim = queries.shape[4]
    scores = jnp.einsum('bgrtd,bsgd->bgrts', queries, key_vecs, preferred_element_type=jnp.float32) * (head_dim ** -0.5)
    causal = lax.broadcasted_iota(jnp.int32, (seq_len, seq_len), 0) >= lax.broadcasted_iota(jnp.int32, (seq_len, seq_len), 1)
    weights = jax.nn.softmax(jnp.where(causal, scores, MASK_VALUE), axis=-1).astype(jnp.bfloat16)
    return jnp.einsum('bgrts,bsgd->bgrtd', weights, val_vecs, preferred_element_type=jnp.float32).astype(jnp.bfloat16)


def cross_attend(queries, key_vecs, val_vecs, visible):
    batch_len, kv_groups, rep_heads, seq_len, head_dim = queries.shape
    vis_len = key_vecs.shape[1]
    tile_count = visible.shape[2]
    scores = jnp.einsum('bgrtd,bsgd->bgrts', queries, key_vecs, preferred_element_type=jnp.float32) * (head_dim ** -0.5)
    scores = scores.reshape(batch_len, kv_groups, rep_heads, seq_len, tile_count, vis_len // tile_count)
    scores = jnp.where(visible[:, None, None, :, :, None], scores, MASK_VALUE)
    weights = jax.nn.softmax(scores.reshape(batch_len, kv_groups, rep_heads, seq_len, vis_len), axis=-1).astype(jnp.bfloat16)
    return jnp.einsum('bgrts,bsgd->bgrtd', weights, val_vecs, preferred_element_type=jnp.float32).astype(jnp.bfloat16)


MESH = pl.DeviceIdType.MESH
D_SUM, X_ONE, Y_ONE, Y_TWO, X_TWO, X_OWN, Y_OWN, C_OWN, Y_FWD, X_FWD, C_X, C_Y, C_DIAG = range(13)
FLOWS = 13
TILE = 256


def fused_kernel(samples, has_pre, has_post, swiglu, gated, has_aux, n_post, *refs):
    refs = list(refs)
    take = lambda n: [refs.pop(0) for _ in range(n)]
    lhs, w_pre = take(2) if has_pre else (None, None)
    resid, = take(1)
    gate, = take(1) if gated else (None,)
    gain, = take(1) if has_post else (None,)
    w_post = take(n_post)
    aux, = take(1) if has_aux else (None,)
    h_out, = take(1) if has_pre else (None,)
    res, = take(1) if has_post else (None,)
    aux_out, = take(1) if has_aux else (None,)
    if has_pre:
        wv_pre, part, rec_d, acc, rec_x1, rec_y1, two_l, two_h, rec_y2, rec_x2 = take(10)
    wv_post = take(n_post)
    out, = take(1) if has_post else (None,)
    send, recv, wsem = take(3)
    me = lax.axis_index('tp')
    c = me % 2
    x = (me // 2) % 2
    y = me // 4
    pc, px, py = me + 1 - 2 * c, me + 2 - 4 * x, me + 4 - 8 * y
    rows, dim = resid.shape[1:]
    half = dim // 2
    lo, hi = pl.ds(0, half), pl.ds(half, half)

    loads = []
    if has_pre:
        loads.append(pltpu.make_async_copy(w_pre, wv_pre, wsem.at[0]))
    for i in range(n_post):
        loads.append(pltpu.make_async_copy(w_post[i], wv_post[i], wsem.at[1 + i]))
    for ld in loads:
        ld.start()

    def slot(s, dy, dx, dc):
        return out.at[s, (1 - y) if dy else y, (1 - x) if dx else x, (1 - c) if dc else c]

    def ends(flow, s):
        if flow == D_SUM:
            return part.at[s, :, :, 1 - c], rec_d.at[s], pc, rec_d.at[s]
        if flow == X_ONE:
            return acc.at[s, :, 1 - x, :, lo], rec_x1.at[s], px, rec_x1.at[s]
        if flow == Y_ONE:
            return acc.at[s, 1 - y, :, :, hi], rec_y1.at[s], py, rec_y1.at[s]
        if flow == Y_TWO:
            return two_l.at[s, 1 - y], rec_y2.at[s], py, rec_y2.at[s]
        if flow == X_TWO:
            return two_h.at[s, 1 - x], rec_x2.at[s], px, rec_x2.at[s]
        own, sx, sy, sd = slot(s, 0, 0, 0), slot(s, 0, 1, 0), slot(s, 1, 0, 0), slot(s, 1, 1, 0)
        if flow == X_OWN:
            return own, own, px, sx
        if flow == Y_OWN:
            return own, own, py, sy
        if flow == C_OWN:
            return own, own, pc, slot(s, 0, 0, 1)
        if flow == Y_FWD:
            return sx.at[:, lo], sx.at[:, lo], py, sd.at[:, lo]
        if flow == X_FWD:
            return sy.at[:, hi], sy.at[:, hi], px, sd.at[:, hi]
        if flow == C_X:
            return sx, sx, pc, slot(s, 0, 1, 1)
        if flow == C_Y:
            return sy, sy, pc, slot(s, 1, 0, 1)
        return sd, sd, pc, slot(s, 1, 1, 1)

    def descr(flow, s, incoming):
        src, dst, who, landing = ends(flow, s)
        return pltpu.make_async_remote_copy(src_ref=src, dst_ref=landing if incoming else dst, send_sem=send.at[flow, s], recv_sem=recv.at[flow, s], device_id={'tp': who}, device_id_type=MESH)

    def start(flow, s):
        descr(flow, s, False).start()

    def got(flow, s):
        descr(flow, s, True).wait_recv()

    def f32(value):
        return value.astype(jnp.float32)

    def normed(values):
        mean_sq = jnp.mean(values * values, axis=-1, keepdims=True)
        return (values * lax.rsqrt(mean_sq + NORM_EPS) * f32(gain[...])).astype(jnp.bfloat16)

    barrier = pltpu.get_barrier_semaphore()
    peers = [lax.rem(me + k, 8) for k in range(1, 8)] if has_aux else [pc, px, py]
    for who in peers:
        pl.semaphore_signal(barrier, inc=1, device_id={'tp': who}, device_id_type=MESH)
    pl.semaphore_wait(barrier, len(peers))

    aux_sent = []
    if has_aux:
        aux_send, aux_recv = take(2)
        aux_out[me] = aux[...]
        for k in range(1, 8):
            cp = pltpu.make_async_remote_copy(src_ref=aux, dst_ref=aux_out.at[me], send_sem=aux_send.at[k], recv_sem=aux_recv.at[k], device_id={'tp': lax.rem(me + k, 8)}, device_id_type=MESH)
            cp.start()
            aux_sent.append(cp)

    def st_pre(s):
        @pl.when(s == 0)
        def _():
            loads[0].wait()
        left = lhs[s]
        for n in range(dim // TILE):
            cols = pl.ds(n * TILE, TILE)
            prod = jnp.dot(left, wv_pre[:, cols], preferred_element_type=jnp.float32)
            part[s, :, :, :, :, cols] = prod.astype(jnp.bfloat16).reshape(2, 2, 2, rows, TILE)
        start(D_SUM, s)

    def st_r1(s):
        got(D_SUM, s)
        acc[s] = (f32(part[s, :, :, c]) + f32(rec_d[s])).astype(jnp.bfloat16)
        start(X_ONE, s)
        start(Y_ONE, s)

    def st_r2(s):
        got(X_ONE, s)
        two_l[s] = (f32(acc[s, :, x, :, lo]) + f32(rec_x1[s])).astype(jnp.bfloat16)
        start(Y_TWO, s)
        got(Y_ONE, s)
        two_h[s] = (f32(acc[s, y, :, :, hi]) + f32(rec_y1[s])).astype(jnp.bfloat16)
        start(X_TWO, s)

    def st_r3(s):
        got(Y_TWO, s)
        got(X_TWO, s)
        total = jnp.concatenate([f32(two_l[s, y]) + f32(rec_y2[s]), f32(two_h[s, x]) + f32(rec_x2[s])], axis=-1)
        if gated:
            total = total * gate[s]
        new = (f32(resid[s]) + total).astype(jnp.bfloat16)
        h_out[s] = new
        if has_post:
            out[s, y, x, c] = normed(f32(new))
            for flow in (X_OWN, Y_OWN, C_OWN):
                start(flow, s)

    def st_g1(s):
        out[s, y, x, c] = normed(f32(resid[s]))
        for flow in (X_OWN, Y_OWN, C_OWN):
            start(flow, s)

    def st_g2(s):
        got(X_OWN, s)
        start(Y_FWD, s)
        start(C_X, s)
        got(Y_OWN, s)
        start(X_FWD, s)
        start(C_Y, s)

    def st_g3(s):
        got(Y_FWD, s)
        got(X_FWD, s)
        start(C_DIAG, s)

    def st_g4(s):
        for flow in (C_OWN, C_X, C_Y, C_DIAG):
            got(flow, s)

        @pl.when(s == 0)
        def _():
            for ld in loads[len(loads) - n_post:]:
                ld.wait()
        left = out[s].reshape(8 * rows, dim)
        if swiglu:
            for n in range(res.shape[-1] // TILE):
                cols = pl.ds(n * TILE, TILE)
                gate_proj = jnp.dot(left, wv_post[0][:, cols], preferred_element_type=jnp.float32)
                up_proj = jnp.dot(left, wv_post[1][:, cols], preferred_element_type=jnp.float32)
                res[s, :, cols] = (jax.nn.silu(gate_proj) * up_proj).astype(jnp.bfloat16)
        else:
            base = 0
            for w in wv_post:
                for n in range(w.shape[-1] // TILE):
                    res[s, :, pl.ds(base, TILE)] = jnp.dot(left, w[:, pl.ds(n * TILE, TILE)], preferred_element_type=jnp.float32)
                    base += TILE

    flows, stages = [], []
    if has_pre:
        stages += [st_pre, st_r1, st_r2, st_r3]
        flows += [D_SUM, X_ONE, Y_ONE, Y_TWO, X_TWO]
    else:
        stages += [st_g1]
    if has_post:
        stages += [st_g2, st_g3, st_g4]
        flows += [X_OWN, Y_OWN, C_OWN, Y_FWD, X_FWD, C_X, C_Y, C_DIAG]

    def step(t, carry):
        for k, stage in enumerate(stages):
            s = t - k

            @pl.when((s >= 0) & (s < samples))
            def _(stage=stage, s=s):
                stage(s)
        return carry

    lax.fori_loop(0, samples + len(stages) - 1, step, 0)

    def drain(s, carry):
        for flow in flows:
            descr(flow, s, False).wait_send()
        return carry

    lax.fori_loop(0, samples, drain, 0)
    for k in range(1, 8 if has_aux else 1):
        src = lax.rem(me + 8 - k, 8)
        pltpu.make_async_remote_copy(src_ref=aux, dst_ref=aux_out.at[src], send_sem=aux_send.at[k], recv_sem=aux_recv.at[k], device_id={'tp': pc}, device_id_type=MESH).wait_recv()
    for cp in aux_sent:
        cp.wait_send()


def fused(cid, resid, lhs=None, w_pre=None, gate=None, gain=None, w_post=(), swiglu=False, aux=None):
    samples, rows, dim = resid.shape
    bf16 = jnp.bfloat16
    half = dim // 2
    has_pre, has_post = lhs is not None, gain is not None
    vmem = pl.BlockSpec(memory_space=pltpu.VMEM)
    hbm = pl.BlockSpec(memory_space=pl.ANY)
    args, specs, outs, scratch = [], [], [], []

    def add(value, spec):
        args.append(value)
        specs.append(spec)

    flops = 0
    if has_pre:
        add(lhs, vmem)
        add(w_pre, hbm)
        flops += 2 * samples * 8 * rows * w_pre.size
        outs.append(jax.ShapeDtypeStruct(resid.shape, bf16))
        scratch += [
            pltpu.VMEM(w_pre.shape, bf16),
            pltpu.VMEM((samples, 2, 2, 2, rows, dim), bf16),
            pltpu.VMEM((samples, 2, 2, rows, dim), bf16), pltpu.VMEM((samples, 2, 2, rows, dim), bf16),
            pltpu.VMEM((samples, 2, rows, half), bf16), pltpu.VMEM((samples, 2, rows, half), bf16),
            pltpu.VMEM((samples, 2, rows, half), bf16), pltpu.VMEM((samples, 2, rows, half), bf16),
            pltpu.VMEM((samples, rows, half), bf16), pltpu.VMEM((samples, rows, half), bf16)]
    add(resid, vmem)
    if gate is not None:
        add(gate, vmem)
    if has_post:
        add(gain.reshape(1, dim), vmem)
        for w in w_post:
            add(w, hbm)
            flops += 2 * samples * 8 * rows * w.size
            scratch.append(pltpu.VMEM(w.shape, bf16))
        if swiglu:
            outs.append(jax.ShapeDtypeStruct((samples, 8 * rows, w_post[0].shape[1]), bf16))
        else:
            outs.append(jax.ShapeDtypeStruct((samples, 8 * rows, sum(w.shape[1] for w in w_post)), jnp.float32))
        scratch.append(pltpu.VMEM((samples, 2, 2, 2, rows, dim), bf16))
    if aux is not None:
        add(aux, vmem)
        outs.append(jax.ShapeDtypeStruct((8,) + aux.shape, aux.dtype))
    scratch += [pltpu.SemaphoreType.DMA((FLOWS, samples)), pltpu.SemaphoreType.DMA((FLOWS, samples)), pltpu.SemaphoreType.DMA((1 + len(w_post),))]
    if aux is not None:
        scratch += [pltpu.SemaphoreType.DMA((8,)), pltpu.SemaphoreType.DMA((8,))]
    return pl.pallas_call(
        functools.partial(fused_kernel, samples, has_pre, has_post, swiglu, gate is not None, aux is not None, len(w_post)),
        out_shape=tuple(outs), in_specs=specs, out_specs=tuple([vmem] * len(outs)),
        scratch_shapes=scratch, name=f'fused_{cid}',
        cost_estimate=pl.CostEstimate(flops=flops + 2 * 10 ** 10, bytes_accessed=10 ** 7, transcendentals=0),
        compiler_params=pltpu.CompilerParams(collective_id=cid, has_side_effects=True, vmem_limit_bytes=67043328),
    )(*args)


Q_X, Q_Y, Q_YF, Q_XF, O_X1, O_Y1, O_Y2, O_X2 = range(8)
STAT = 8


def cross_kernel(samples, q_ref, k_hbm, v_hbm, vis_ref, ctx, q_all, k_vm, v_vm, ob_l, ob_h, rec_x1, rec_y1, two_l, two_h, rec_y2, rec_x2, send, recv, ksem):
    me = lax.axis_index('tp')
    x = (me // 2) % 2
    y = me // 4
    px, py = me + 2 - 4 * x, me + 4 - 8 * y
    rows, size = q_ref.shape[1:]
    top, low = pl.ds(0, rows // 2), pl.ds(rows // 2, rows // 2)
    half = size // 2
    scale = size ** -0.5
    loads = [pltpu.make_async_copy(k_hbm, k_vm, ksem.at[0]), pltpu.make_async_copy(v_hbm, v_vm, ksem.at[1])]
    for ld in loads:
        ld.start()

    def ends(flow, s):
        own, sx, sy, sd = q_all.at[s, y, x], q_all.at[s, y, 1 - x], q_all.at[s, 1 - y, x], q_all.at[s, 1 - y, 1 - x]
        if flow == Q_X:
            return own, own, px, sx
        if flow == Q_Y:
            return own, own, py, sy
        if flow == Q_YF:
            return sx.at[top], sx.at[top], py, sd.at[top]
        if flow == Q_XF:
            return sy.at[low], sy.at[low], px, sd.at[low]
        if flow == O_X1:
            return ob_l.at[s, :, 1 - x], rec_x1.at[s], px, rec_x1.at[s]
        if flow == O_Y1:
            return ob_h.at[s, 1 - y], rec_y1.at[s], py, rec_y1.at[s]
        if flow == O_Y2:
            return two_l.at[s, 1 - y], rec_y2.at[s], py, rec_y2.at[s]
        return two_h.at[s, 1 - x], rec_x2.at[s], px, rec_x2.at[s]

    def descr(flow, s, incoming):
        src, dst, who, landing = ends(flow, s)
        return pltpu.make_async_remote_copy(src_ref=src, dst_ref=landing if incoming else dst, send_sem=send.at[flow, s], recv_sem=recv.at[flow, s], device_id={'tp': who}, device_id_type=MESH)

    def start(flow, s):
        descr(flow, s, False).start()

    def got(flow, s):
        descr(flow, s, True).wait_recv()

    barrier = pltpu.get_barrier_semaphore()
    for who in (px, py):
        pl.semaphore_signal(barrier, inc=1, device_id={'tp': who}, device_id_type=MESH)
    pl.semaphore_wait(barrier, 2)

    def stat_block(top_row, sum_row):
        return jnp.concatenate([top_row, sum_row] + [top_row] * (STAT - 2), axis=0)

    def merged(a, b):
        max_a, max_b = a[half:half + 1], b[half:half + 1]
        peak = jnp.maximum(max_a, max_b)
        fac_a, fac_b = jnp.exp(max_a - peak), jnp.exp(max_b - peak)
        total = a[half + 1:half + 2] * fac_a + b[half + 1:half + 2] * fac_b
        return a[:half] * fac_a + b[:half] * fac_b, peak, total

    def st_a(s):
        q_all[s, y, x] = q_ref[s]
        start(Q_X, s)
        start(Q_Y, s)

    def st_b(s):
        got(Q_X, s)
        start(Q_YF, s)
        got(Q_Y, s)
        start(Q_XF, s)

    def st_c(s):
        got(Q_YF, s)
        got(Q_XF, s)

        @pl.when(s == 0)
        def _():
            for ld in loads:
                ld.wait()
        seen = vis_ref[s] > 0
        for p in range(4):
            cols = pl.ds(p * size, size)
            keys = k_vm[:, s, :, cols].reshape(-1, size)
            vals = v_vm[:, s, :, cols].reshape(-1, size)
            scores = lax.dot_general(keys, q_all[s, p // 2, p % 2], (((1,), (1,)), ((), ())), preferred_element_type=jnp.float32) * scale
            scores = jnp.where(seen, scores, MASK_VALUE)
            peak = jnp.max(scores, axis=0, keepdims=True)
            weights = jnp.exp(scores - peak)
            total = jnp.sum(weights, axis=0, keepdims=True)
            context = lax.dot_general(vals, weights.astype(jnp.bfloat16), (((0,), (0,)), ((), ())), preferred_element_type=jnp.float32)
            stats = stat_block(peak, total)
            ob_l[s, p // 2, p % 2, :half] = context[:half]
            ob_h[s, p // 2, p % 2, :half] = context[half:]
            ob_l[s, p // 2, p % 2, half:] = stats
            ob_h[s, p // 2, p % 2, half:] = stats
        start(O_X1, s)
        start(O_Y1, s)

    def st_d(s):
        got(O_X1, s)
        for q in range(2):
            body, peak, total = merged(ob_l[s, q, x], rec_x1[s, q])
            two_l[s, q, :half] = body
            two_l[s, q, half:] = stat_block(peak, total)
        start(O_Y2, s)
        got(O_Y1, s)
        for q in range(2):
            body, peak, total = merged(ob_h[s, y, q], rec_y1[s, q])
            two_h[s, q, :half] = body
            two_h[s, q, half:] = stat_block(peak, total)
        start(O_X2, s)

    def st_e(s):
        got(O_Y2, s)
        got(O_X2, s)
        parts = []
        for mine, other in ((two_l[s, y], rec_y2[s]), (two_h[s, x], rec_x2[s])):
            body, _, total = merged(mine, other)
            parts.append(body / total)
        whole = jnp.concatenate(parts, axis=0).T.astype(jnp.bfloat16)
        reps = rows // ctx.shape[1]
        for r in range(reps):
            ctx[s, :, r * size:(r + 1) * size] = whole[r * ctx.shape[1]:(r + 1) * ctx.shape[1]]

    stages = [st_a, st_b, st_c, st_d, st_e]

    def step(t, carry):
        for k, stage in enumerate(stages):
            s = t - k

            @pl.when((s >= 0) & (s < samples))
            def _(stage=stage, s=s):
                stage(s)
        return carry

    lax.fori_loop(0, samples + len(stages) - 1, step, 0)

    def drain(s, carry):
        for flow in range(8):
            descr(flow, s, False).wait_send()
        return carry

    lax.fori_loop(0, samples, drain, 0)


def cross(cid, queries, keys, vals, seen, tokens):
    samples, rows, size = queries.shape
    f32, bf16 = jnp.float32, jnp.bfloat16
    half = size // 2
    vmem = pl.BlockSpec(memory_space=pltpu.VMEM)
    hbm = pl.BlockSpec(memory_space=pl.ANY)
    wide = pltpu.VMEM((samples, 2, half + STAT, rows), f32)
    one = pltpu.VMEM((samples, half + STAT, rows), f32)
    both = pltpu.VMEM((samples, 2, 2, half + STAT, rows), f32)
    return pl.pallas_call(
        functools.partial(cross_kernel, samples),
        out_shape=jax.ShapeDtypeStruct((samples, tokens, rows // tokens * size), bf16),
        in_specs=[vmem, hbm, hbm, vmem], out_specs=vmem,
        scratch_shapes=[
            pltpu.VMEM((samples, 2, 2, rows, size), bf16), pltpu.VMEM(keys.shape, bf16), pltpu.VMEM(vals.shape, bf16),
            both, both, wide, wide, wide, wide, one, one,
            pltpu.SemaphoreType.DMA((8, samples)), pltpu.SemaphoreType.DMA((8, samples)), pltpu.SemaphoreType.DMA((2,))],
        name=f'cross_{cid}',
        cost_estimate=pl.CostEstimate(flops=5 * 10 ** 10, bytes_accessed=10 ** 7, transcendentals=0),
        compiler_params=pltpu.CompilerParams(collective_id=cid, has_side_effects=True, vmem_limit_bytes=60 * 2 ** 20),
    )(queries, keys, vals, seen)


def kv_kernel(head_dim, own_ref, par_ref, wk_ref, wv_ref, gain_ref, k_ref, v_ref):
    for i, src in enumerate((own_ref, par_ref)):
        rows = src[0]
        for n in range(wk_ref.shape[1] // head_dim):
            cols = pl.ds(n * head_dim, head_dim)
            keys = jnp.dot(rows, wk_ref[:, cols], preferred_element_type=jnp.float32)
            mean_sq = jnp.mean(keys * keys, axis=-1, keepdims=True)
            k_ref[i, 0, :, cols] = (keys * lax.rsqrt(mean_sq + NORM_EPS) * gain_ref[...].astype(jnp.float32)).astype(jnp.bfloat16)
            v_ref[i, 0, :, cols] = jnp.dot(rows, wv_ref[:, cols], preferred_element_type=jnp.float32).astype(jnp.bfloat16)


def project_kv(own, partner, wk, wv, gain):
    samples, rows, dim = own.shape
    width = wk.shape[1]
    rows_spec = pl.BlockSpec((1, rows, dim), lambda s: (s, 0, 0))
    weight_spec = pl.BlockSpec((dim, width), lambda s: (0, 0))
    out_spec = pl.BlockSpec((2, 1, rows, width), lambda s: (0, s, 0, 0))
    out = jax.ShapeDtypeStruct((2, samples, rows, width), jnp.bfloat16)
    return pl.pallas_call(
        functools.partial(kv_kernel, gain.shape[0]), grid=(samples,),
        in_specs=[rows_spec, rows_spec, weight_spec, weight_spec, pl.BlockSpec((1, gain.shape[0]), lambda s: (0, 0))],
        out_specs=(out_spec, out_spec), out_shape=(out, out), name='project_kv',
        cost_estimate=pl.CostEstimate(flops=8 * samples * rows * dim * width, bytes_accessed=10 ** 8, transcendentals=0),
        compiler_params=pltpu.CompilerParams(vmem_limit_bytes=60 * 2 ** 20),
    )(own, partner, wk, wv, gain.reshape(1, -1))


def solution(mesh):
    act_spec = P('dp', 'tp', None)
    col_spec = P(None, 'tp')
    row_spec = P('tp', None)
    layer_a = (P(), col_spec, col_spec, col_spec, row_spec, P(), col_spec, col_spec, row_spec)
    layer_b = (P(), col_spec, P(), col_spec, col_spec, P(), row_spec, P(), col_spec, col_spec, row_spec, P())
    in_specs = (act_spec, act_spec, P('dp', 'tp'), act_spec) + layer_a + layer_b

    def body(hidden, vision, positions, tile_mask, ln1_a, wq_a, wk_a, wv_a, wo_a, ln2_a, wg_a, wu_a, wd_a, ln1_b, wq_b, q_norm, wk_b, wv_b, k_norm, wo_b, ln2_b, wg_b, wu_b, wd_b, xgates):
        me = lax.axis_index('tp')
        head_dim = q_norm.shape[0]
        samples, rows, model_dim = hidden.shape
        tokens = rows * 8
        tiles = tile_mask.shape[2]
        kv_local = wk_a.shape[1] // head_dim
        rep_heads = wq_a.shape[1] // head_dim // kv_local

        same_core = [[core + 2 * chip for chip in range(4)] for core in range(2)]
        wk_all = lax.all_gather(wk_b, 'tp', axis=1, tiled=True, axis_index_groups=same_core)
        wv_all = lax.all_gather(wv_b, 'tp', axis=1, tiled=True, axis_index_groups=same_core)
        vis_partner = lax.ppermute(vision, 'tp', [(i, i ^ 1) for i in range(8)])

        small = jnp.concatenate([positions.reshape(-1), tile_mask.reshape(-1)])
        aux = jnp.pad(small, (0, 1024 - small.shape[0])).reshape(8, 128)
        proj, aux_all = fused(1, hidden, gain=ln1_a, w_post=(wq_a, wk_a, wv_a), aux=aux)
        aux_all = aux_all.reshape(8, 1024)
        pos_all = aux_all[:, :samples * rows].reshape(8, samples, rows).transpose(1, 0, 2).reshape(samples, tokens)
        mask_all = aux_all[:, samples * rows:samples * rows * (1 + tiles)].reshape(8, samples, rows, tiles).transpose(1, 0, 2, 3).reshape(samples, tokens, tiles)

        angles = pos_all.astype(jnp.float32)[..., None] * rope_table(head_dim)
        cos_tab = jnp.cos(angles)[:, :, None, :]
        sin_tab = jnp.sin(angles)[:, :, None, :]
        proj = proj.reshape(samples, tokens, rep_heads + 2, head_dim)
        rotated = rotate(proj[:, :, :rep_heads + 1], cos_tab, sin_tab).astype(jnp.bfloat16)
        queries = rotated[:, :, :rep_heads].transpose(0, 2, 1, 3)[:, None]
        context = self_attend(queries, rotated[:, :, rep_heads:], proj[:, :, rep_heads + 1:].astype(jnp.bfloat16))
        context = context[:, 0].transpose(0, 2, 1, 3).reshape(samples, tokens, rep_heads * head_dim)
        h_one, act = fused(2, hidden, lhs=context, w_pre=wo_a, gain=ln2_a, w_post=(wg_a, wu_a), swiglu=True)
        h_two, queries = fused(3, h_one, lhs=act, w_pre=wd_a, gain=ln1_b, w_post=(wq_b,))
        queries = rms_scale(queries.reshape(samples, tokens, rep_heads, head_dim), q_norm).astype(jnp.bfloat16)
        queries = queries.transpose(0, 2, 1, 3).reshape(samples, rep_heads * tokens, head_dim)
        keys, vals = project_kv(vision, vis_partner, wk_all, wv_all, k_norm)
        seen = jnp.tile(lax.dynamic_index_in_dim(mask_all, me // 2, axis=2, keepdims=False)[:, None, :], (1, 1, rep_heads))
        context = cross(6, queries, keys, vals, seen, tokens)
        row_keep = jnp.any(tile_mask > 0, axis=-1, keepdims=True).astype(jnp.float32)
        gate_vals = jnp.tanh(xgates.astype(jnp.float32))
        h_three, act = fused(4, h_two, lhs=context, w_pre=wo_b, gate=gate_vals[0] * row_keep, gain=ln2_b, w_post=(wg_b, wu_b), swiglu=True)
        return fused(5, h_three, lhs=act, w_pre=wd_b, gate=gate_vals[1] * row_keep)[0]

    return jax.shard_map(body, mesh=mesh, in_specs=in_specs, out_specs=act_spec, check_vma=False)
```

```python
import functools
import math
import jax
import jax.numpy as jnp
from jax import lax
from jax.experimental import pallas as pl
from jax.experimental.pallas import tpu as pltpu
from jax.sharding import PartitionSpec as P

ROPE_THETA = 500000.0
ROPE_FACTOR = 8.0
LOW_FACTOR = 1.0
HIGH_FACTOR = 4.0
ORIG_CONTEXT = 8192.0
NORM_EPS = 1e-5
MASK_VALUE = -1e30


def rope_table(head_dim):
    low_wave = ORIG_CONTEXT / LOW_FACTOR
    high_wave = ORIG_CONTEXT / HIGH_FACTOR
    freq_list = []
    for freq_idx in range(head_dim // 2):
        base_freq = 1.0 / (ROPE_THETA ** (2.0 * freq_idx / head_dim))
        wave_len = 2.0 * math.pi / base_freq
        if wave_len > low_wave:
            freq_list.append(base_freq / ROPE_FACTOR)
        elif wave_len < high_wave:
            freq_list.append(base_freq)
        else:
            smooth = (ORIG_CONTEXT / wave_len - LOW_FACTOR) / (HIGH_FACTOR - LOW_FACTOR)
            freq_list.append((1.0 - smooth) * base_freq / ROPE_FACTOR + smooth * base_freq)
    return jnp.array(freq_list, dtype=jnp.float32)


def rms_scale(values, norm_gain):
    values = values.astype(jnp.float32)
    mean_sq = jnp.mean(values * values, axis=-1, keepdims=True)
    return values * lax.rsqrt(mean_sq + NORM_EPS) * norm_gain.astype(jnp.float32)


def rotate(values, cos_tab, sin_tab):
    half_dim = values.shape[-1] // 2
    first_half = values[..., :half_dim]
    second_half = values[..., half_dim:]
    return jnp.concatenate([first_half * cos_tab - second_half * sin_tab, second_half * cos_tab + first_half * sin_tab], axis=-1)


def self_attend(queries, key_vecs, val_vecs):
    seq_len = queries.shape[3]
    head_dim = queries.shape[4]
    scores = jnp.einsum('bgrtd,bsgd->bgrts', queries, key_vecs, preferred_element_type=jnp.float32) * (head_dim ** -0.5)
    causal = lax.broadcasted_iota(jnp.int32, (seq_len, seq_len), 0) >= lax.broadcasted_iota(jnp.int32, (seq_len, seq_len), 1)
    weights = jax.nn.softmax(jnp.where(causal, scores, MASK_VALUE), axis=-1).astype(jnp.bfloat16)
    return jnp.einsum('bgrts,bsgd->bgrtd', weights, val_vecs, preferred_element_type=jnp.float32).astype(jnp.bfloat16)


def cross_attend(queries, key_vecs, val_vecs, visible):
    batch_len, kv_groups, rep_heads, seq_len, head_dim = queries.shape
    vis_len = key_vecs.shape[1]
    tile_count = visible.shape[2]
    scores = jnp.einsum('bgrtd,bsgd->bgrts', queries, key_vecs, preferred_element_type=jnp.float32) * (head_dim ** -0.5)
    scores = scores.reshape(batch_len, kv_groups, rep_heads, seq_len, tile_count, vis_len // tile_count)
    scores = jnp.where(visible[:, None, None, :, :, None], scores, MASK_VALUE)
    weights = jax.nn.softmax(scores.reshape(batch_len, kv_groups, rep_heads, seq_len, vis_len), axis=-1).astype(jnp.bfloat16)
    return jnp.einsum('bgrts,bsgd->bgrtd', weights, val_vecs, preferred_element_type=jnp.float32).astype(jnp.bfloat16)


MESH = pl.DeviceIdType.MESH
D_SUM, X_ONE, Y_ONE, Y_TWO, X_TWO, X_OWN, Y_OWN, C_OWN, Y_FWD, X_FWD, C_X, C_Y, C_DIAG = range(13)
FLOWS = 13
TILE = 256
CHUNK = 112


def fused_kernel(samples, has_pre, has_post, mode, gated, has_aux, has_attn, n_post, gain_row, near_part, has_far, *refs):
    refs = list(refs)
    take = lambda n: [refs.pop(0) for _ in range(n)]
    lhs, w_pre = take(2) if has_pre else (None, None)
    cos, sin = take(2) if has_attn else (None, None)
    q_gain, = take(1) if mode == 'queries' else (None,)
    resid, = take(1)
    gate, = take(1) if gated else (None,)
    gain, = take(1) if has_post else (None,)
    w_post = take(n_post)
    aux, = take(1) if has_aux else (None,)
    own_w = take(2) if near_part is not None else None
    far_src, = take(1) if has_far else (None,)
    h_out, = take(1) if has_pre else (None,)
    res, = take(1) if has_post else (None,)
    aux_out, = take(1) if has_aux else (None,)
    near_out, = take(1) if near_part is not None else (None,)
    far_out, = take(1) if has_far else (None,)
    if has_pre:
        wv_pre, part, rec_d, acc, rec_x1, rec_y1, two_l, two_h, rec_y2, rec_x2 = take(10)
    wv_post = take(n_post)
    out, = take(1) if has_post else (None,)
    send, recv, wsem = take(3)
    near_send, near_recv, fwd_send, fwd_recv = take(4) if near_part is not None else (None,) * 4
    far_send, far_recv = take(2) if has_far else (None, None)
    me = lax.axis_index('tp')
    c = me % 2
    x = (me // 2) % 2
    y = me // 4
    pc, px, py = me + 1 - 2 * c, me + 2 - 4 * x, me + 4 - 8 * y
    z = lax.axis_index('dp')
    pz = z + 1 - 2 * (z % 2)
    rows, dim = resid.shape[1:]
    half = dim // 2
    lo, hi = pl.ds(0, half), pl.ds(half, half)

    loads = []
    if has_pre:
        loads.append(pltpu.make_async_copy(w_pre, wv_pre, wsem.at[0]))
    for i in range(n_post):
        loads.append(pltpu.make_async_copy(w_post[i], wv_post[i], wsem.at[1 + i]))
    for ld in loads:
        ld.start()

    def slot(s, dy, dx, dc):
        return out.at[s, (1 - y) if dy else y, (1 - x) if dx else x, (1 - c) if dc else c]

    def ends(flow, s):
        if flow == D_SUM:
            return part.at[s, :, :, 1 - c], rec_d.at[s], pc, rec_d.at[s]
        if flow == X_ONE:
            return acc.at[s, :, 1 - x, :, lo], rec_x1.at[s], px, rec_x1.at[s]
        if flow == Y_ONE:
            return acc.at[s, 1 - y, :, :, hi], rec_y1.at[s], py, rec_y1.at[s]
        if flow == Y_TWO:
            return two_l.at[s, 1 - y], rec_y2.at[s], py, rec_y2.at[s]
        if flow == X_TWO:
            return two_h.at[s, 1 - x], rec_x2.at[s], px, rec_x2.at[s]
        own, sx, sy, sd = slot(s, 0, 0, 0), slot(s, 0, 1, 0), slot(s, 1, 0, 0), slot(s, 1, 1, 0)
        if flow == X_OWN:
            return own, own, px, sx
        if flow == Y_OWN:
            return own, own, py, sy
        if flow == C_OWN:
            return own, own, pc, slot(s, 0, 0, 1)
        if flow == Y_FWD:
            return sx.at[:, lo], sx.at[:, lo], py, sd.at[:, lo]
        if flow == X_FWD:
            return sy.at[:, hi], sy.at[:, hi], px, sd.at[:, hi]
        if flow == C_X:
            return sx, sx, pc, slot(s, 0, 1, 1)
        if flow == C_Y:
            return sy, sy, pc, slot(s, 1, 0, 1)
        return sd, sd, pc, slot(s, 1, 1, 1)

    def descr(flow, s, incoming):
        src, dst, who, landing = ends(flow, s)
        return pltpu.make_async_remote_copy(src_ref=src, dst_ref=landing if incoming else dst, send_sem=send.at[flow, s], recv_sem=recv.at[flow, s], device_id={'tp': who}, device_id_type=MESH)

    def start(flow, s):
        descr(flow, s, False).start()

    def got(flow, s):
        descr(flow, s, True).wait_recv()

    def f32(value):
        return value.astype(jnp.float32)

    def normed(values):
        mean_sq = jnp.mean(values * values, axis=-1, keepdims=True)
        return (values * lax.rsqrt(mean_sq + NORM_EPS) * f32(gain[gain_row:gain_row + 1])).astype(jnp.bfloat16)

    barrier = pltpu.get_barrier_semaphore()
    peers = [lax.rem(me + k, 8) for k in range(1, 8)] if has_aux else [pc, px, py]
    for who in peers:
        pl.semaphore_signal(barrier, inc=1, device_id={'tp': who}, device_id_type=MESH)
    if has_far:
        pl.semaphore_signal(barrier, inc=1, device_id={'dp': pz}, device_id_type=MESH)
    pl.semaphore_wait(barrier, len(peers) + (1 if has_far else 0))

    part_rows = near_out.shape[2] if near_part is not None else 0
    chunks = part_rows // CHUNK

    def near_copy(p, kind, j):
        first = part_rows * (2 * near_part + z % 2) + j * CHUNK
        return pltpu.make_async_remote_copy(src_ref=own_w[kind].at[pl.ds(pl.multiple_of(first, CHUNK), CHUNK)], dst_ref=near_out.at[p, kind, pl.ds(j * CHUNK, CHUNK)], send_sem=near_send.at[p, kind, j], recv_sem=near_recv.at[p, kind, j], device_id={'tp': (px, py)[p]}, device_id_type=MESH)

    def fwd_copy(p, j):
        span = pl.ds(j * CHUNK, CHUNK)
        return pltpu.make_async_remote_copy(src_ref=near_out.at[p, :, span], dst_ref=near_out.at[2, :, span], send_sem=fwd_send.at[j], recv_sem=fwd_recv.at[j], device_id={'tp': (py, px)[p]}, device_id_type=MESH)

    def chunk_send(j):
        for p in range(2):
            for kind in range(2):
                near_copy(p, kind, j).start()

    def chunk_forward(j):
        for p in range(2):
            for kind in range(2):
                near_copy(p, kind, j).wait_recv()
        for p in range(2):
            @pl.when(j % 2 == p)
            def _(p=p):
                fwd_copy(p, j).start()

    far_copy = None
    if has_far:
        far_copy = pltpu.make_async_remote_copy(src_ref=far_src, dst_ref=far_out, send_sem=far_send, recv_sem=far_recv, device_id={'dp': pz}, device_id_type=MESH)
        far_copy.start()

    aux_sent = []
    if has_aux:
        aux_send, aux_recv = take(2)
        aux_out[me] = aux[...]
        for k in range(1, 8):
            cp = pltpu.make_async_remote_copy(src_ref=aux, dst_ref=aux_out.at[me], send_sem=aux_send.at[k], recv_sem=aux_recv.at[k], device_id={'tp': lax.rem(me + k, 8)}, device_id_type=MESH)
            cp.start()
            aux_sent.append(cp)

    def self_attention(s):
        size = 2 * cos.shape[-1]
        heads = lhs.shape[-1] // size - 2
        cos_tab, sin_tab = cos[s], sin[s]

        def head(i):
            return lhs[s, :, i * size:(i + 1) * size]

        keys = rotate(head(heads), cos_tab, sin_tab).astype(jnp.bfloat16)
        vals = head(heads + 1).astype(jnp.bfloat16)
        length = keys.shape[0]
        causal = lax.broadcasted_iota(jnp.int32, (length, length), 0) >= lax.broadcasted_iota(jnp.int32, (length, length), 1)
        parts = []
        for i in range(heads):
            query = rotate(head(i), cos_tab, sin_tab).astype(jnp.bfloat16)
            scores = lax.dot_general(query, keys, (((1,), (1,)), ((), ())), preferred_element_type=jnp.float32) * (size ** -0.5)
            scores = jnp.where(causal, scores, MASK_VALUE)
            weights = jnp.exp(scores - jnp.max(scores, axis=-1, keepdims=True))
            weights = (weights / jnp.sum(weights, axis=-1, keepdims=True)).astype(jnp.bfloat16)
            parts.append(jnp.dot(weights, vals, preferred_element_type=jnp.float32).astype(jnp.bfloat16))
        return jnp.concatenate(parts, axis=-1)

    def st_pre(s):
        @pl.when(s == 0)
        def _():
            loads[0].wait()
        left = self_attention(s) if has_attn else lhs[s]
        for n in range(dim // TILE):
            cols = pl.ds(n * TILE, TILE)
            prod = jnp.dot(left, wv_pre[:, cols], preferred_element_type=jnp.float32)
            part[s, :, :, :, :, cols] = prod.astype(jnp.bfloat16).reshape(2, 2, 2, rows, TILE)
        start(D_SUM, s)

    def st_r1(s):
        got(D_SUM, s)
        acc[s] = (f32(part[s, :, :, c]) + f32(rec_d[s])).astype(jnp.bfloat16)
        start(X_ONE, s)
        start(Y_ONE, s)

    def st_r2(s):
        got(X_ONE, s)
        two_l[s] = (f32(acc[s, :, x, :, lo]) + f32(rec_x1[s])).astype(jnp.bfloat16)
        start(Y_TWO, s)
        got(Y_ONE, s)
        two_h[s] = (f32(acc[s, y, :, :, hi]) + f32(rec_y1[s])).astype(jnp.bfloat16)
        start(X_TWO, s)

    def st_r3(s):
        got(Y_TWO, s)
        got(X_TWO, s)
        total = jnp.concatenate([f32(two_l[s, y]) + f32(rec_y2[s]), f32(two_h[s, x]) + f32(rec_x2[s])], axis=-1)
        if gated:
            total = total * gate[s]
        new = (f32(resid[s]) + total).astype(jnp.bfloat16)
        h_out[s] = new
        if has_post:
            out[s, y, x, c] = normed(f32(new))
            for flow in (X_OWN, Y_OWN, C_OWN):
                start(flow, s)

    def st_g1(s):
        out[s, y, x, c] = normed(f32(resid[s]))
        for flow in (X_OWN, Y_OWN, C_OWN):
            start(flow, s)

    def st_g2(s):
        got(X_OWN, s)
        start(Y_FWD, s)
        start(C_X, s)
        got(Y_OWN, s)
        start(X_FWD, s)
        start(C_Y, s)

    def st_g3(s):
        got(Y_FWD, s)
        got(X_FWD, s)
        start(C_DIAG, s)

    def st_g4(s):
        for flow in (C_OWN, C_X, C_Y, C_DIAG):
            got(flow, s)

        @pl.when(s == 0)
        def _():
            for ld in loads[len(loads) - n_post:]:
                ld.wait()
        left = out[s].reshape(8 * rows, dim)
        if mode == 'swiglu':
            for n in range(res.shape[-1] // TILE):
                cols = pl.ds(n * TILE, TILE)
                gate_proj = jnp.dot(left, wv_post[0][:, cols], preferred_element_type=jnp.float32)
                up_proj = jnp.dot(left, wv_post[1][:, cols], preferred_element_type=jnp.float32)
                res[s, :, cols] = (jax.nn.silu(gate_proj) * up_proj).astype(jnp.bfloat16)
        elif mode == 'queries':
            length, size = left.shape[0], q_gain.shape[-1]
            for n in range(wv_post[0].shape[-1] // size):
                prod = jnp.dot(left, wv_post[0][:, pl.ds(n * size, size)], preferred_element_type=jnp.float32)
                mean_sq = jnp.mean(prod * prod, axis=-1, keepdims=True)
                res[s, n * length:(n + 1) * length] = (prod * lax.rsqrt(mean_sq + NORM_EPS) * f32(q_gain[0:1])).astype(jnp.bfloat16)
        else:
            base = 0
            for w in wv_post:
                for n in range(w.shape[-1] // TILE):
                    res[s, :, pl.ds(base, TILE)] = jnp.dot(left, w[:, pl.ds(n * TILE, TILE)], preferred_element_type=jnp.float32)
                    base += TILE

    flows, stages = [], []
    if has_pre:
        stages += [st_pre, st_r1, st_r2, st_r3]
        flows += [D_SUM, X_ONE, Y_ONE, Y_TWO, X_TWO]
    else:
        stages += [st_g1]
    if has_post:
        stages += [st_g2, st_g3, st_g4]
        flows += [X_OWN, Y_OWN, C_OWN, Y_FWD, X_FWD, C_X, C_Y, C_DIAG]

    def step(t, carry):
        for k, stage in enumerate(stages):
            s = t - k

            @pl.when((s >= 0) & (s < samples))
            def _(stage=stage, s=s):
                stage(s)
        if chunks:
            for action, lag in ((chunk_forward, 2), (chunk_send, 0)):
                j = t - lag

                @pl.when((j >= 0) & (j < chunks))
                def _(action=action, j=j):
                    action(j)
        return carry

    lax.fori_loop(0, max(samples + len(stages) - 1, chunks + 2), step, 0)

    def drain(s, carry):
        for flow in flows:
            descr(flow, s, False).wait_send()
        return carry

    lax.fori_loop(0, samples, drain, 0)

    def finish(j, carry):
        for p in range(2):
            for kind in range(2):
                near_copy(p, kind, j).wait_send()
        fwd_copy(0, j).wait()
        return carry

    if chunks:
        lax.fori_loop(0, chunks, finish, 0)
    if has_far:
        far_copy.wait()
    for k in range(1, 8 if has_aux else 1):
        src = lax.rem(me + 8 - k, 8)
        pltpu.make_async_remote_copy(src_ref=aux, dst_ref=aux_out.at[src], send_sem=aux_send.at[k], recv_sem=aux_recv.at[k], device_id={'tp': pc}, device_id_type=MESH).wait_recv()
    for cp in aux_sent:
        cp.wait_send()


def fused(cid, resid, lhs=None, w_pre=None, gate=None, gain=None, w_post=(), mode=None, aux=None, rope=None, q_gain=None, gain_row=0, mine=None, near_part=None, far_src=None):
    samples, rows, dim = resid.shape
    bf16 = jnp.bfloat16
    half = dim // 2
    has_pre, has_post = lhs is not None, gain is not None
    vmem = pl.BlockSpec(memory_space=pltpu.VMEM)
    hbm = pl.BlockSpec(memory_space=pl.ANY)
    args, specs, outs, scratch = [], [], [], []

    def add(value, spec):
        args.append(value)
        specs.append(spec)

    flops = 0
    if has_pre:
        add(lhs, vmem)
        add(w_pre, hbm)
        flops += 2 * samples * 8 * rows * w_pre.size
        outs.append(jax.ShapeDtypeStruct(resid.shape, bf16))
        scratch += [
            pltpu.VMEM(w_pre.shape, bf16),
            pltpu.VMEM((samples, 2, 2, 2, rows, dim), bf16),
            pltpu.VMEM((samples, 2, 2, rows, dim), bf16), pltpu.VMEM((samples, 2, 2, rows, dim), bf16),
            pltpu.VMEM((samples, 2, rows, half), bf16), pltpu.VMEM((samples, 2, rows, half), bf16),
            pltpu.VMEM((samples, 2, rows, half), bf16), pltpu.VMEM((samples, 2, rows, half), bf16),
            pltpu.VMEM((samples, rows, half), bf16), pltpu.VMEM((samples, rows, half), bf16)]
    if rope is not None:
        add(rope[0], vmem)
        add(rope[1], vmem)
    if q_gain is not None:
        add(q_gain, vmem)
    add(resid, vmem)
    if gate is not None:
        add(gate, vmem)
    if has_post:
        add(gain, vmem)
        for w in w_post:
            add(w, hbm)
            flops += 2 * samples * 8 * rows * w.size
            scratch.append(pltpu.VMEM(w.shape, bf16))
        if mode == 'swiglu':
            outs.append(jax.ShapeDtypeStruct((samples, 8 * rows, w_post[0].shape[1]), bf16))
        elif mode == 'queries':
            size = q_gain.shape[1]
            outs.append(jax.ShapeDtypeStruct((samples, 8 * rows * (w_post[0].shape[1] // size), size), bf16))
        else:
            outs.append(jax.ShapeDtypeStruct((samples, 8 * rows, sum(w.shape[1] for w in w_post)), jnp.float32))
        scratch.append(pltpu.VMEM((samples, 2, 2, 2, rows, dim), bf16))
    if aux is not None:
        add(aux, vmem)
        outs.append(jax.ShapeDtypeStruct((8,) + aux.shape, aux.dtype))
    if near_part is not None:
        add(mine[0], hbm)
        add(mine[1], hbm)
        part_shape = (2, mine[0].shape[0] // 4, mine[0].shape[1])
    if far_src is not None:
        add(far_src, hbm)
    out_specs = [vmem] * len(outs)
    if near_part is not None:
        outs.append(jax.ShapeDtypeStruct((3,) + part_shape, bf16))
    if far_src is not None:
        outs.append(jax.ShapeDtypeStruct(far_src.shape, bf16))
    out_specs += [hbm] * (len(outs) - len(out_specs))
    scratch += [pltpu.SemaphoreType.DMA((FLOWS, samples)), pltpu.SemaphoreType.DMA((FLOWS, samples)), pltpu.SemaphoreType.DMA((1 + len(w_post),))]
    if near_part is not None:
        scratch += [pltpu.SemaphoreType.DMA((2, 2, part_shape[1] // CHUNK))] * 2 + [pltpu.SemaphoreType.DMA((part_shape[1] // CHUNK,))] * 2
    if far_src is not None:
        scratch += [pltpu.SemaphoreType.DMA] * 2
    if aux is not None:
        scratch += [pltpu.SemaphoreType.DMA((8,)), pltpu.SemaphoreType.DMA((8,))]
    return pl.pallas_call(
        functools.partial(fused_kernel, samples, has_pre, has_post, mode, gate is not None, aux is not None, rope is not None, len(w_post), gain_row, near_part, far_src is not None),
        out_shape=tuple(outs), in_specs=specs, out_specs=tuple(out_specs),
        scratch_shapes=scratch, name=f'fused_{cid}',
        cost_estimate=pl.CostEstimate(flops=flops + 2 * 10 ** 10, bytes_accessed=10 ** 7, transcendentals=0),
        compiler_params=pltpu.CompilerParams(collective_id=cid, has_side_effects=True, vmem_limit_bytes=67043328),
    )(*args)


Q_X, Q_Y, Q_YF, Q_XF, O_X1, O_Y1, O_Y2, O_X2 = range(8)
STAT = 8


def cross_kernel(samples, n_w, q_ref, seen_ref, gain_ref, own_hbm, par_hbm, *refs):
    w_hbm, refs = refs[:n_w], refs[n_w:]
    ctx, q_all, w_vm, vis_vm, k_vm, v_vm, ob_l, ob_h, rec_x1, rec_y1, two_l, two_h, rec_y2, rec_x2, send, recv, wsem, vsem = refs
    me = lax.axis_index('tp')
    z = lax.axis_index('dp')
    x = (me // 2) % 2
    y = me // 4
    px, py = me + 2 - 4 * x, me + 4 - 8 * y
    rows, size = q_ref.shape[1:]
    vis_rows = own_hbm.shape[1]
    top, low = pl.ds(0, rows // 2), pl.ds(rows // 2, rows // 2)
    half = size // 2
    scale = size ** -0.5
    sources = [w_hbm[0], w_hbm[1]]
    targets = [w_vm.at[0, :, pl.ds(0, size)], w_vm.at[0, :, pl.ds(size, size)]]
    part = w_hbm[2].shape[2]
    for i, ref in enumerate(w_hbm[2:]):
        base = part * (2 * (i // 2) + (z + i) % 2)
        for p in range(3):
            for kind in range(2):
                sources.append(ref.at[p, kind])
                targets.append(w_vm.at[1 + p, pl.ds(base, part), pl.ds(kind * size, size)])
    loads = [pltpu.make_async_copy(src, dst, wsem.at[i]) for i, (src, dst) in enumerate(zip(sources, targets))]

    def vis_loads(s):
        spot = s % 2
        return [pltpu.make_async_copy(src.at[s], vis_vm.at[spot, i], vsem.at[spot, i]) for i, src in enumerate((own_hbm, par_hbm))]

    for ld in vis_loads(0):
        ld.start()
    for ld in loads:
        ld.start()

    def near(ref, s, p):
        return ref.at[s, (1 - y) if p // 2 else y, (1 - x) if p % 2 else x]

    def ends(flow, s):
        own, sx, sy, sd = q_all.at[s, y, x], q_all.at[s, y, 1 - x], q_all.at[s, 1 - y, x], q_all.at[s, 1 - y, 1 - x]
        if flow == Q_X:
            return own, own, px, sx
        if flow == Q_Y:
            return own, own, py, sy
        if flow == Q_YF:
            return sx.at[top], sx.at[top], py, sd.at[top]
        if flow == Q_XF:
            return sy.at[low], sy.at[low], px, sd.at[low]
        if flow == O_X1:
            return ob_l.at[s, :, 1 - x], rec_x1.at[s], px, rec_x1.at[s]
        if flow == O_Y1:
            return ob_h.at[s, 1 - y], rec_y1.at[s], py, rec_y1.at[s]
        if flow == O_Y2:
            return two_l.at[s, 1 - y], rec_y2.at[s], py, rec_y2.at[s]
        return two_h.at[s, 1 - x], rec_x2.at[s], px, rec_x2.at[s]

    def descr(flow, s, incoming):
        src, dst, who, landing = ends(flow, s)
        return pltpu.make_async_remote_copy(src_ref=src, dst_ref=landing if incoming else dst, send_sem=send.at[flow, s], recv_sem=recv.at[flow, s], device_id={'tp': who}, device_id_type=MESH)

    def start(flow, s):
        descr(flow, s, False).start()

    def got(flow, s):
        descr(flow, s, True).wait_recv()

    barrier = pltpu.get_barrier_semaphore()
    for who in (px, py):
        pl.semaphore_signal(barrier, inc=1, device_id={'tp': who}, device_id_type=MESH)
    pl.semaphore_wait(barrier, 2)

    def stat_block(top_row, sum_row):
        return jnp.concatenate([top_row, sum_row] + [top_row] * (STAT - 2), axis=0)

    def merged(a, b):
        max_a, max_b = a[half:half + 1], b[half:half + 1]
        peak = jnp.maximum(max_a, max_b)
        fac_a, fac_b = jnp.exp(max_a - peak), jnp.exp(max_b - peak)
        total = a[half + 1:half + 2] * fac_a + b[half + 1:half + 2] * fac_b
        return a[:half] * fac_a + b[:half] * fac_b, peak, total

    def st_a(s):
        q_all[s, y, x] = q_ref[s]
        start(Q_X, s)
        start(Q_Y, s)

    def st_b(s):
        got(Q_X, s)
        start(Q_YF, s)
        got(Q_Y, s)
        start(Q_XF, s)

    def st_c(s):
        got(Q_YF, s)
        got(Q_XF, s)
        seen = seen_ref[s] > 0
        spot = s % 2
        for p in range(4):
            cols = pl.ds(p * size, size)
            keys = k_vm[spot, :, cols]
            vals = v_vm[spot, :, cols]
            scores = lax.dot_general(keys, near(q_all, s, p)[...], (((1,), (1,)), ((), ())), preferred_element_type=jnp.float32) * scale
            scores = jnp.where(seen, scores, MASK_VALUE)
            peak = jnp.max(scores, axis=0, keepdims=True)
            weights = jnp.exp(scores - peak)
            total = jnp.sum(weights, axis=0, keepdims=True)
            context = lax.dot_general(vals, weights.astype(jnp.bfloat16), (((0,), (0,)), ((), ())), preferred_element_type=jnp.float32)
            stats = stat_block(peak, total)
            for ref, part in ((ob_l, context[:half]), (ob_h, context[half:])):
                near(ref, s, p)[:half] = part
                near(ref, s, p)[half:] = stats
        start(O_X1, s)
        start(O_Y1, s)

    def st_d(s):
        got(O_X1, s)
        for q in range(2):
            body, peak, total = merged(ob_l[s, q, x], rec_x1[s, q])
            two_l[s, q, :half] = body
            two_l[s, q, half:] = stat_block(peak, total)
        start(O_Y2, s)
        got(O_Y1, s)
        for q in range(2):
            body, peak, total = merged(ob_h[s, y, q], rec_y1[s, q])
            two_h[s, q, :half] = body
            two_h[s, q, half:] = stat_block(peak, total)
        start(O_X2, s)

    def st_e(s):
        got(O_Y2, s)
        got(O_X2, s)
        parts = []
        for mine, other in ((two_l[s, y], rec_y2[s]), (two_h[s, x], rec_x2[s])):
            body, _, total = merged(mine, other)
            parts.append(body / total)
        whole = jnp.concatenate(parts, axis=0).T.astype(jnp.bfloat16)
        reps = rows // ctx.shape[1]
        for r in range(reps):
            ctx[s, :, r * size:(r + 1) * size] = whole[r * ctx.shape[1]:(r + 1) * ctx.shape[1]]

    def st_j(s):
        @pl.when(s == 0)
        def _():
            for ld in loads:
                ld.wait()

        @pl.when(s + 1 < samples)
        def _():
            for ld in vis_loads(s + 1):
                ld.start()
        for ld in vis_loads(s):
            ld.wait()
        spot = s % 2
        rows_in = vis_vm[spot].reshape(2 * vis_rows, -1)
        for p in range(4):
            cols = pl.ds(p * size, size)
            keys = jnp.dot(rows_in, w_vm[p, :, pl.ds(0, size)], preferred_element_type=jnp.float32)
            mean_sq = jnp.mean(keys * keys, axis=-1, keepdims=True)
            k_vm[spot, :, cols] = (keys * lax.rsqrt(mean_sq + NORM_EPS) * gain_ref[1:2].astype(jnp.float32)).astype(jnp.bfloat16)
            v_vm[spot, :, cols] = jnp.dot(rows_in, w_vm[p, :, pl.ds(size, size)], preferred_element_type=jnp.float32).astype(jnp.bfloat16)

    stages = [(st_d, 2), (st_e, 3), (st_c, 1), (st_b, 0), (st_j, 0)]

    def step(t, carry):
        for stage, lag in stages:
            s = t - lag

            @pl.when((s >= 0) & (s < samples))
            def _(stage=stage, s=s):
                stage(s)
        return carry

    def first(s, carry):
        st_a(s)
        return carry

    lax.fori_loop(0, samples, first, 0)
    lax.fori_loop(0, samples + 3, step, 0)

    def drain(s, carry):
        for flow in range(8):
            descr(flow, s, False).wait_send()
        return carry

    lax.fori_loop(0, samples, drain, 0)


def cross(cid, queries, seen, gain, own, partner, weights, tokens):
    samples, rows, size = queries.shape
    vis_rows, dim = own.shape[1:]
    f32, bf16 = jnp.float32, jnp.bfloat16
    half = size // 2
    vmem = pl.BlockSpec(memory_space=pltpu.VMEM)
    hbm = pl.BlockSpec(memory_space=pl.ANY)
    wide = pltpu.VMEM((samples, 2, half + STAT, rows), f32)
    one = pltpu.VMEM((samples, half + STAT, rows), f32)
    both = pltpu.VMEM((samples, 2, 2, half + STAT, rows), f32)
    heads = pltpu.VMEM((2, 2 * vis_rows, 4 * size), bf16)
    return pl.pallas_call(
        functools.partial(cross_kernel, samples, len(weights)),
        out_shape=jax.ShapeDtypeStruct((samples, tokens, rows // tokens * size), bf16),
        in_specs=[vmem, vmem, vmem] + [hbm] * (2 + len(weights)), out_specs=vmem,
        scratch_shapes=[
            pltpu.VMEM((samples, 2, 2, rows, size), bf16), pltpu.VMEM((4, dim, 2 * size), bf16),
            pltpu.VMEM((2, 2, vis_rows, dim), bf16), heads, heads,
            both, both, wide, wide, wide, wide, one, one,
            pltpu.SemaphoreType.DMA((8, samples)), pltpu.SemaphoreType.DMA((8, samples)),
            pltpu.SemaphoreType.DMA((26,)), pltpu.SemaphoreType.DMA((2, 2))],
        name=f'cross_{cid}',
        cost_estimate=pl.CostEstimate(flops=8 * 10 ** 10, bytes_accessed=10 ** 7, transcendentals=0),
        compiler_params=pltpu.CompilerParams(collective_id=cid, has_side_effects=True, vmem_limit_bytes=60 * 2 ** 20),
    )(queries, seen, gain, own, partner, *weights)


def solution(mesh):
    act_spec = P('dp', 'tp', None)
    col_spec = P(None, 'tp')
    row_spec = P('tp', None)
    layer_a = (P(), col_spec, col_spec, col_spec, row_spec, P(), col_spec, col_spec, row_spec)
    layer_b = (P(), col_spec, P(), col_spec, col_spec, P(), row_spec, P(), col_spec, col_spec, row_spec, P())
    in_specs = (act_spec, act_spec, P('dp', 'tp'), act_spec) + layer_a + layer_b

    def body(hidden, vision, positions, tile_mask, ln1_a, wq_a, wk_a, wv_a, wo_a, ln2_a, wg_a, wu_a, wd_a, ln1_b, wq_b, q_norm, wk_b, wv_b, k_norm, wo_b, ln2_b, wg_b, wu_b, wd_b, xgates):
        me = lax.axis_index('tp')
        head_dim = q_norm.shape[0]
        samples, rows, model_dim = hidden.shape
        tokens = rows * 8
        tiles = tile_mask.shape[2]
        kv_local = wk_a.shape[1] // head_dim
        rep_heads = wq_a.shape[1] // head_dim // kv_local

        gains = jnp.stack([ln1_a, ln2_a, ln1_b, ln2_b])
        head_gains = jnp.stack([q_norm, k_norm])
        vis_partner = lax.ppermute(vision, 'tp', [(i, i ^ 1) for i in range(8)])

        small = jnp.concatenate([positions.reshape(-1), tile_mask.reshape(-1)])
        aux = jnp.pad(small, (0, 1024 - small.shape[0])).reshape(8, 128)
        proj, aux_all, near_one = fused(1, hidden, gain=gains, gain_row=0, w_post=(wq_a, wk_a, wv_a), aux=aux, mine=(wk_b, wv_b), near_part=0)
        aux_all = aux_all.reshape(8, 1024)
        pos_all = aux_all[:, :samples * rows].reshape(8, samples, rows).transpose(1, 0, 2).reshape(samples, tokens)
        mask_all = aux_all[:, samples * rows:samples * rows * (1 + tiles)].reshape(8, samples, rows, tiles).transpose(1, 0, 2, 3).reshape(samples, tokens, tiles)

        angles = pos_all.astype(jnp.float32)[..., None] * rope_table(head_dim)
        rope = (jnp.cos(angles), jnp.sin(angles))
        h_one, act, near_two, far_one = fused(2, hidden, lhs=proj, w_pre=wo_a, rope=rope, gain=gains, gain_row=1, w_post=(wg_a, wu_a), mode='swiglu', mine=(wk_b, wv_b), near_part=1, far_src=near_one)
        h_two, queries, far_two = fused(3, h_one, lhs=act, w_pre=wd_a, gain=gains, gain_row=2, w_post=(wq_b,), mode='queries', q_gain=head_gains, far_src=near_two)
        weights = (wk_b, wv_b, near_one, far_one, near_two, far_two)
        seen = jnp.tile(lax.dynamic_index_in_dim(mask_all, me // 2, axis=2, keepdims=False)[:, None, :], (1, 1, rep_heads))
        context = cross(6, queries, seen, head_gains, vision, vis_partner, weights, tokens)
        row_keep = jnp.any(tile_mask > 0, axis=-1, keepdims=True).astype(jnp.float32)
        gate_vals = jnp.tanh(xgates.astype(jnp.float32))
        h_three, act = fused(4, h_two, lhs=context, w_pre=wo_b, gate=gate_vals[0] * row_keep, gain=gains, gain_row=3, w_post=(wg_b, wu_b), mode='swiglu')
        return fused(5, h_three, lhs=act, w_pre=wd_b, gate=gate_vals[1] * row_keep)[0]

    return jax.shard_map(body, mesh=mesh, in_specs=in_specs, out_specs=act_spec, check_vma=False)
```

```python
import functools
import math
import jax
import jax.numpy as jnp
from jax import lax
from jax.experimental import pallas as pl
from jax.experimental.pallas import tpu as pltpu
from jax.sharding import PartitionSpec as P

ROPE_THETA = 500000.0
ROPE_FACTOR = 8.0
LOW_FACTOR = 1.0
HIGH_FACTOR = 4.0
ORIG_CONTEXT = 8192.0
NORM_EPS = 1e-5
MASK_VALUE = -1e30


def rope_table(head_dim):
    low_wave = ORIG_CONTEXT / LOW_FACTOR
    high_wave = ORIG_CONTEXT / HIGH_FACTOR
    freq_list = []
    for freq_idx in range(head_dim // 2):
        base_freq = 1.0 / (ROPE_THETA ** (2.0 * freq_idx / head_dim))
        wave_len = 2.0 * math.pi / base_freq
        if wave_len > low_wave:
            freq_list.append(base_freq / ROPE_FACTOR)
        elif wave_len < high_wave:
            freq_list.append(base_freq)
        else:
            smooth = (ORIG_CONTEXT / wave_len - LOW_FACTOR) / (HIGH_FACTOR - LOW_FACTOR)
            freq_list.append((1.0 - smooth) * base_freq / ROPE_FACTOR + smooth * base_freq)
    return jnp.array(freq_list, dtype=jnp.float32)


def rotate(values, cos_tab, sin_tab):
    half_dim = values.shape[-1] // 2
    first_half = values[..., :half_dim]
    second_half = values[..., half_dim:]
    return jnp.concatenate([first_half * cos_tab - second_half * sin_tab, second_half * cos_tab + first_half * sin_tab], axis=-1)


MESH = pl.DeviceIdType.MESH
D_SUM, X_ONE, Y_ONE, Y_TWO, X_TWO, X_OWN, Y_OWN, C_OWN, Y_FWD, X_FWD, C_X, C_Y, C_DIAG = range(13)
FLOWS = 13
TILE = 256
PLANE = (2, 2)
CUBE = (2, 2, 2)
CHUNKS = (112, 112)
CHUNK_PAUSE = ((8, 0), (3, 4))


def given(value):
    return value is not None


def fused_kernel(samples, has_pre, has_post, mode, gate_row, has_aux, has_attn, n_post, gain_row, near_part, has_far, has_kv, *refs):
    refs = list(refs)
    one = lambda held: refs.pop(0) if held else None
    take = lambda n, held=True: [one(held) for _ in range(n)]
    lhs, w_pre = take(2, has_pre)
    cos, sin = take(2, has_attn)
    q_gain = one(mode == 'queries')
    vis_src, kv_w = take(2, has_kv), take(2, has_kv)
    resid = one(True)
    tile_mask, xgates = take(2, given(gate_row))
    gain = one(has_post)
    w_post = take(n_post)
    aux = one(has_aux)
    own_w = take(2, given(near_part))
    far_src = one(has_far)
    h_out = one(has_pre)
    res = one(has_post)
    aux_out = one(has_aux)
    kv_out = one(has_kv)
    near_out = one(given(near_part))
    far_out = one(has_far)
    if has_pre:
        wv_pre, part, rec_d, acc, rec_x1, rec_y1, two_l, two_h, rec_y2, rec_x2 = take(10)
    wv_post = take(n_post)
    out = one(has_post)
    gate = one(given(gate_row))
    vis_vm, kv_vm, vis_sem, kv_sem = take(4, has_kv)
    send, recv, wsem = take(3)
    near_send, near_recv, fwd_send, fwd_recv = take(4, given(near_part))
    far_send, far_recv = take(2, has_far)
    me = lax.axis_index('tp')
    c = me % 2
    x = (me // 2) % 2
    y = me // 4
    pc, px, py = me + 1 - 2 * c, me + 2 - 4 * x, me + 4 - 8 * y
    z = lax.axis_index('dp')
    pz = z + 1 - 2 * (z % 2)
    rows, dim = resid.shape[1:]
    half = dim // 2
    lo, hi = pl.ds(0, half), pl.ds(half, half)

    loads = []
    if has_pre:
        for i, span in enumerate((lo, hi)):
            loads.append(pltpu.make_async_copy(w_pre.at[:, span], wv_pre.at[:, span], wsem.at[i]))
    for i in range(n_post):
        loads.append(pltpu.make_async_copy(w_post[i], wv_post[i], wsem.at[2 + i]))
    for ld in loads:
        ld.start()

    def vis_loads(s):
        return [pltpu.make_async_copy(src.at[s], vis_vm.at[s % 2, i], vis_sem.at[s % 2, i]) for i, src in enumerate(vis_src)]

    kv_loads = []
    if has_kv:
        size = kv_w[0].shape[1]
        kv_loads = [pltpu.make_async_copy(src, kv_vm.at[:, pl.ds(i * size, size)], kv_sem.at[i]) for i, src in enumerate(kv_w)]
        for ld in kv_loads + vis_loads(0):
            ld.start()

    def st_kv(s):
        @pl.when(s == 0)
        def _():
            for ld in kv_loads:
                ld.wait()

        @pl.when(s + 1 < samples)
        def _():
            for ld in vis_loads(s + 1):
                ld.start()
        for ld in vis_loads(s):
            ld.wait()
        rows_in = vis_vm[s % 2].reshape(-1, dim)
        keys = jnp.dot(rows_in, kv_vm[:, pl.ds(0, size)], preferred_element_type=jnp.float32)
        mean_sq = jnp.mean(keys * keys, axis=-1, keepdims=True)
        kv_out[s, :, pl.ds(0, size)] = (keys * lax.rsqrt(mean_sq + NORM_EPS) * f32(q_gain[1:2])).astype(jnp.bfloat16)
        kv_out[s, :, pl.ds(size, size)] = jnp.dot(rows_in, kv_vm[:, pl.ds(size, size)], preferred_element_type=jnp.float32).astype(jnp.bfloat16)

    def slot(s, dy, dx, dc):
        return out.at[s, (1 - y) if dy else y, (1 - x) if dx else x, (1 - c) if dc else c]

    def ends(flow, s):
        if flow == D_SUM:
            return part.at[s, :, :, 1 - c], rec_d.at[s], pc, rec_d.at[s]
        if flow == X_ONE:
            return acc.at[s, :, 1 - x, :, lo], rec_x1.at[s], px, rec_x1.at[s]
        if flow == Y_ONE:
            return acc.at[s, 1 - y, :, :, hi], rec_y1.at[s], py, rec_y1.at[s]
        if flow == Y_TWO:
            return two_l.at[s, 1 - y], rec_y2.at[s], py, rec_y2.at[s]
        if flow == X_TWO:
            return two_h.at[s, 1 - x], rec_x2.at[s], px, rec_x2.at[s]
        own, sx, sy, sd = slot(s, 0, 0, 0), slot(s, 0, 1, 0), slot(s, 1, 0, 0), slot(s, 1, 1, 0)
        if flow == X_OWN:
            return own, own, px, sx
        if flow == Y_OWN:
            return own, own, py, sy
        if flow == C_OWN:
            return own, own, pc, slot(s, 0, 0, 1)
        if flow == Y_FWD:
            return sx.at[:, lo], sx.at[:, lo], py, sd.at[:, lo]
        if flow == X_FWD:
            return sy.at[:, hi], sy.at[:, hi], px, sd.at[:, hi]
        if flow == C_X:
            return sx, sx, pc, slot(s, 0, 1, 1)
        if flow == C_Y:
            return sy, sy, pc, slot(s, 1, 0, 1)
        return sd, sd, pc, slot(s, 1, 1, 1)

    def descr(flow, s, incoming):
        src, dst, who, landing = ends(flow, s)
        return pltpu.make_async_remote_copy(src_ref=src, dst_ref=landing if incoming else dst, send_sem=send.at[flow, s], recv_sem=recv.at[flow, s], device_id={'tp': who}, device_id_type=MESH)

    def start(flow, s):
        descr(flow, s, False).start()

    def got(flow, s):
        descr(flow, s, True).wait_recv()

    def f32(value):
        return value.astype(jnp.float32)

    def normed(values):
        mean_sq = jnp.mean(values * values, axis=-1, keepdims=True)
        return (values * lax.rsqrt(mean_sq + NORM_EPS) * f32(gain[gain_row:gain_row + 1])).astype(jnp.bfloat16)

    if given(gate_row):
        keep = jnp.where(jnp.max(tile_mask[...], axis=-1, keepdims=True) > 0, 1.0, 0.0)
        gate[...] = jnp.tanh(jnp.full(keep.shape, xgates[gate_row], jnp.float32)) * keep

    barrier = pltpu.get_barrier_semaphore()
    peers = [lax.rem(me + k, 8) for k in range(1, 8)] if has_aux else [pc, px, py]
    for who in peers:
        pl.semaphore_signal(barrier, inc=1, device_id={'tp': who}, device_id_type=MESH)
    if has_far:
        pl.semaphore_signal(barrier, inc=1, device_id={'dp': pz}, device_id_type=MESH)
    pl.semaphore_wait(barrier, len(peers) + (1 if has_far else 0))

    chunk = CHUNKS[near_part or 0]
    part_rows = near_out.shape[2] if given(near_part) else 0
    chunks = part_rows // chunk

    def near_copy(p, kind, j):
        first = part_rows * (2 * near_part + z % 2) + j * chunk
        return pltpu.make_async_remote_copy(src_ref=own_w[kind].at[pl.ds(pl.multiple_of(first, chunk), chunk)], dst_ref=near_out.at[p, kind, pl.ds(j * chunk, chunk)], send_sem=near_send.at[p, kind, j], recv_sem=near_recv.at[p, kind, j], device_id={'tp': (px, py)[p]}, device_id_type=MESH)

    def fwd_copy(p, j):
        span = pl.ds(j * chunk, chunk)
        return pltpu.make_async_remote_copy(src_ref=near_out.at[p, :, span], dst_ref=near_out.at[2, :, span], send_sem=fwd_send.at[j], recv_sem=fwd_recv.at[j], device_id={'tp': (py, px)[p]}, device_id_type=MESH)

    def chunk_send(j):
        for p in range(2):
            for kind in range(2):
                near_copy(p, kind, j).start()

    def chunk_forward(j):
        for p in range(2):
            for kind in range(2):
                near_copy(p, kind, j).wait_recv()
        for p in range(2):
            @pl.when(j % 2 == p)
            def _(p=p):
                fwd_copy(p, j).start()

    far_copy = None
    if has_far:
        far_copy = pltpu.make_async_remote_copy(src_ref=far_src, dst_ref=far_out, send_sem=far_send, recv_sem=far_recv, device_id={'dp': pz}, device_id_type=MESH)
        far_copy.start()

    aux_sent = []
    if has_aux:
        aux_send, aux_recv = take(2)
        aux_out[me] = aux[...]
        for k in range(1, 8):
            cp = pltpu.make_async_remote_copy(src_ref=aux, dst_ref=aux_out.at[me], send_sem=aux_send.at[k], recv_sem=aux_recv.at[k], device_id={'tp': lax.rem(me + k, 8)}, device_id_type=MESH)
            cp.start()
            aux_sent.append(cp)

    def self_attention(s):
        size = 2 * cos.shape[-1]
        heads = lhs.shape[-1] // size - 2
        cos_tab, sin_tab = cos[s], sin[s]

        def head(i):
            return lhs[s, :, i * size:(i + 1) * size]

        keys = rotate(head(heads), cos_tab, sin_tab).astype(jnp.bfloat16)
        vals = head(heads + 1).astype(jnp.bfloat16)
        length = keys.shape[0]
        causal = lax.broadcasted_iota(jnp.int32, (length, length), 0) >= lax.broadcasted_iota(jnp.int32, (length, length), 1)
        parts = []
        for i in range(heads):
            query = rotate(head(i), cos_tab, sin_tab).astype(jnp.bfloat16)
            scores = lax.dot_general(query, keys, (((1,), (1,)), ((), ())), preferred_element_type=jnp.float32) * (size ** -0.5)
            scores = jnp.where(causal, scores, MASK_VALUE)
            weights = jnp.exp(scores - jnp.max(scores, axis=-1, keepdims=True))
            weights = (weights / jnp.sum(weights, axis=-1, keepdims=True)).astype(jnp.bfloat16)
            parts.append(jnp.dot(weights, vals, preferred_element_type=jnp.float32).astype(jnp.bfloat16))
        return jnp.concatenate(parts, axis=-1)

    def st_pre(s):
        left = self_attention(s) if has_attn else lhs[s]
        for n in range(dim // TILE):
            if n * TILE % half == 0:
                @pl.when(s == 0)
                def _(n=n):
                    loads[n * TILE // half].wait()
            cols = pl.ds(n * TILE, TILE)
            prod = jnp.dot(left, wv_pre[:, cols], preferred_element_type=jnp.float32)
            part[s, :, :, :, :, cols] = prod.astype(jnp.bfloat16).reshape(2, 2, 2, rows, TILE)
        start(D_SUM, s)

    def st_r1(s):
        got(D_SUM, s)
        acc[s] = (f32(part[s, :, :, c]) + f32(rec_d[s])).astype(jnp.bfloat16)
        start(X_ONE, s)
        start(Y_ONE, s)

    def st_r2(s):
        got(X_ONE, s)
        two_l[s] = (f32(acc[s, :, x, :, lo]) + f32(rec_x1[s])).astype(jnp.bfloat16)
        start(Y_TWO, s)
        got(Y_ONE, s)
        two_h[s] = (f32(acc[s, y, :, :, hi]) + f32(rec_y1[s])).astype(jnp.bfloat16)
        start(X_TWO, s)

    def st_r3(s):
        got(Y_TWO, s)
        got(X_TWO, s)
        total = jnp.concatenate([f32(two_l[s, y]) + f32(rec_y2[s]), f32(two_h[s, x]) + f32(rec_x2[s])], axis=-1)
        if given(gate_row):
            total = total * gate[s]
        new = (f32(resid[s]) + total).astype(jnp.bfloat16)
        h_out[s] = new
        if has_post:
            out[s, y, x, c] = normed(f32(new))
            for flow in (X_OWN, Y_OWN, C_OWN):
                start(flow, s)

    def st_g1(s):
        out[s, y, x, c] = normed(f32(resid[s]))
        for flow in (X_OWN, Y_OWN, C_OWN):
            start(flow, s)

    def st_g2(s):
        got(X_OWN, s)
        start(Y_FWD, s)
        start(C_X, s)
        got(Y_OWN, s)
        start(X_FWD, s)
        start(C_Y, s)

    def st_g3(s):
        got(Y_FWD, s)
        got(X_FWD, s)
        start(C_DIAG, s)

    def st_g4(s):
        for flow in (C_OWN, C_X, C_Y, C_DIAG):
            got(flow, s)

        @pl.when(s == 0)
        def _():
            for ld in loads[len(loads) - n_post:]:
                ld.wait()
        left = out[s].reshape(8 * rows, dim)
        if mode == 'swiglu':
            for n in range(res.shape[-1] // TILE):
                cols = pl.ds(n * TILE, TILE)
                gate_proj = jnp.dot(left, wv_post[0][:, cols], preferred_element_type=jnp.float32)
                up_proj = jnp.dot(left, wv_post[1][:, cols], preferred_element_type=jnp.float32)
                res[s, :, cols] = (jax.nn.silu(gate_proj) * up_proj).astype(jnp.bfloat16)
        elif mode == 'queries':
            length, size = left.shape[0], q_gain.shape[-1]
            for n in range(wv_post[0].shape[-1] // size):
                prod = jnp.dot(left, wv_post[0][:, pl.ds(n * size, size)], preferred_element_type=jnp.float32)
                mean_sq = jnp.mean(prod * prod, axis=-1, keepdims=True)
                res[s, n * length:(n + 1) * length] = (prod * lax.rsqrt(mean_sq + NORM_EPS) * f32(q_gain[0:1]) * (size ** -0.5)).astype(jnp.bfloat16)
        else:
            base = 0
            for w in wv_post:
                for n in range(w.shape[-1] // TILE):
                    res[s, :, pl.ds(base, TILE)] = jnp.dot(left, w[:, pl.ds(n * TILE, TILE)], preferred_element_type=jnp.float32)
                    base += TILE

    flows, stages = [], []
    late = 3 if has_pre else 0
    if has_pre:
        stages += [(st_pre, 0), (st_r1, 1), (st_r2, 2), (st_r3, 3)]
        flows += [D_SUM, X_ONE, Y_ONE, Y_TWO, X_TWO]
    else:
        stages += [(st_g1, 0)]
    if has_post:
        stages += [(st_g2, late + 1), (st_g3, late + 2), (st_g4, late + 3)]
        flows += [X_OWN, Y_OWN, C_OWN, Y_FWD, X_FWD, C_X, C_Y, C_DIAG]
    if has_kv:
        stages += [(st_kv, late + 3)]
    steps = samples + max(lag for _, lag in stages)

    def step(t, carry):
        for stage, lag in stages:
            s = t - lag

            @pl.when((s >= 0) & (s < samples))
            def _(stage=stage, s=s):
                stage(s)
        if chunks:
            for action, lag in ((chunk_forward, 2), (chunk_send, 0)):
                early, pause = CHUNK_PAUSE[near_part]
                u = t - lag
                for begin, end, off in ((0, early, 0), (early + pause, chunks + pause, pause)):
                    @pl.when((u >= begin) & (u < end))
                    def _(action=action, j=u - off):
                        action(j)
        return carry

    lax.fori_loop(0, max(steps, chunks + 2 + CHUNK_PAUSE[near_part][1]) if chunks else steps, step, 0)

    def drain(s, carry):
        for flow in flows:
            descr(flow, s, False).wait_send()
        return carry

    lax.fori_loop(0, samples, drain, 0)

    def finish(j, carry):
        for p in range(2):
            for kind in range(2):
                near_copy(p, kind, j).wait_send()
        fwd_copy(0, j).wait()
        return carry

    if chunks:
        lax.fori_loop(0, chunks, finish, 0)
    if has_far:
        far_copy.wait()
    for k in range(1, 8 if has_aux else 1):
        src = lax.rem(me + 8 - k, 8)
        pltpu.make_async_remote_copy(src_ref=aux, dst_ref=aux_out.at[src], send_sem=aux_send.at[k], recv_sem=aux_recv.at[k], device_id={'tp': pc}, device_id_type=MESH).wait_recv()
    for cp in aux_sent:
        cp.wait_send()


def fused(cid, resid, lhs=None, w_pre=None, gate=None, gain=None, w_post=(), mode=None, aux=None, rope=None, q_gain=None, gain_row=0, mine=None, near_part=None, far_src=None, kv=None):
    samples, rows, dim = resid.shape
    bf16 = jnp.bfloat16
    half = dim // 2
    has_pre, has_post = given(lhs), given(gain)
    vmem = pl.BlockSpec(memory_space=pltpu.VMEM)
    hbm = pl.BlockSpec(memory_space=pl.ANY)
    args, specs, outs, scratch = [], [], [], []

    def add(value, spec):
        args.append(value)
        specs.append(spec)

    flops = 0
    if has_pre:
        add(lhs, vmem)
        add(w_pre, hbm)
        flops += 2 * samples * 8 * rows * w_pre.size
        outs.append(jax.ShapeDtypeStruct(resid.shape, bf16))
        scratch += [
            pltpu.VMEM(w_pre.shape, bf16),
            pltpu.VMEM((samples, *CUBE, rows, dim), bf16),
            pltpu.VMEM((samples, *PLANE, rows, dim), bf16), pltpu.VMEM((samples, *PLANE, rows, dim), bf16),
            *[pltpu.VMEM((samples, 2, rows, half), bf16)] * 4,
            *[pltpu.VMEM((samples, rows, half), bf16)] * 2]
    if given(rope):
        add(rope[0], vmem)
        add(rope[1], vmem)
    if given(q_gain):
        add(q_gain, vmem)
    if given(kv):
        for value in kv:
            add(value, hbm)
    add(resid, vmem)
    if given(gate):
        add(gate[0], vmem)
        add(gate[1], pl.BlockSpec(memory_space=pltpu.SMEM))
    if has_post:
        add(gain, vmem)
        for w in w_post:
            add(w, hbm)
            flops += 2 * samples * 8 * rows * w.size
            scratch.append(pltpu.VMEM(w.shape, bf16))
        if mode == 'swiglu':
            outs.append(jax.ShapeDtypeStruct((samples, 8 * rows, w_post[0].shape[1]), bf16))
        elif mode == 'queries':
            size = q_gain.shape[1]
            outs.append(jax.ShapeDtypeStruct((samples, 8 * rows * (w_post[0].shape[1] // size), size), bf16))
        else:
            outs.append(jax.ShapeDtypeStruct((samples, 8 * rows, sum(w.shape[1] for w in w_post)), jnp.float32))
        scratch.append(pltpu.VMEM((samples, *CUBE, rows, dim), bf16))
    if given(aux):
        add(aux, vmem)
        outs.append(jax.ShapeDtypeStruct((8,) + aux.shape, aux.dtype))
    if given(kv):
        outs.append(jax.ShapeDtypeStruct((samples, 2 * kv[0].shape[1], 2 * kv[2].shape[1]), bf16))
    if given(near_part):
        add(mine[0], hbm)
        add(mine[1], hbm)
        part_shape = (2, mine[0].shape[0] // 4, mine[0].shape[1])
    if given(far_src):
        add(far_src, hbm)
    out_specs = [vmem] * len(outs)
    if given(near_part):
        outs.append(jax.ShapeDtypeStruct((3,) + part_shape, bf16))
    if given(far_src):
        outs.append(jax.ShapeDtypeStruct(far_src.shape, bf16))
    out_specs += [hbm] * (len(outs) - len(out_specs))
    if given(gate):
        scratch.append(pltpu.VMEM((samples, rows, 1), jnp.float32))
    if given(kv):
        scratch += [pltpu.VMEM((2, 2) + kv[0].shape[1:], bf16), pltpu.VMEM((dim, 2 * kv[2].shape[1]), bf16), pltpu.SemaphoreType.DMA((2, 2)), pltpu.SemaphoreType.DMA((2,))]
    scratch += [pltpu.SemaphoreType.DMA((FLOWS, samples)), pltpu.SemaphoreType.DMA((FLOWS, samples)), pltpu.SemaphoreType.DMA((2 + len(w_post),))]
    if given(near_part):
        scratch += [pltpu.SemaphoreType.DMA((2, 2, part_shape[1] // CHUNKS[near_part]))] * 2 + [pltpu.SemaphoreType.DMA((part_shape[1] // CHUNKS[near_part],))] * 2
    if given(far_src):
        scratch += [pltpu.SemaphoreType.DMA] * 2
    if given(aux):
        scratch += [pltpu.SemaphoreType.DMA((8,)), pltpu.SemaphoreType.DMA((8,))]
    return pl.pallas_call(
        functools.partial(fused_kernel, samples, has_pre, has_post, mode, gate[2] if given(gate) else None, given(aux), given(rope), len(w_post), gain_row, near_part, given(far_src), given(kv)),
        out_shape=tuple(outs), in_specs=specs, out_specs=tuple(out_specs),
        scratch_shapes=scratch, name=f'fused_{cid}',
        cost_estimate=pl.CostEstimate(flops=flops + 2 * 10 ** 10, bytes_accessed=10 ** 7, transcendentals=0),
        compiler_params=pltpu.CompilerParams(collective_id=cid, has_side_effects=True, vmem_limit_bytes=67043328),
    )(*args)


Q_X, Q_Y, Q_YF, Q_XF, O_X1, O_Y1, O_Y2, O_X2 = range(8)
STAT = 8


def cross_kernel(samples, n_w, q_ref, seen_ref, gain_ref, own_hbm, par_hbm, kv_hbm, *refs):
    w_hbm, refs = refs[:n_w], refs[n_w:]
    ctx, q_all, w_vm, vis_vm, kv_vm, k_vm, v_vm, ob_l, ob_h, rec_x1, rec_y1, two_l, two_h, rec_y2, rec_x2, send, recv, wsem, vsem, kv_sem = refs
    me = lax.axis_index('tp')
    z = lax.axis_index('dp')
    x = (me // 2) % 2
    y = me // 4
    px, py = me + 2 - 4 * x, me + 4 - 8 * y
    rows, size = q_ref.shape[1:]
    vis_rows = own_hbm.shape[1]
    top, low = pl.ds(0, rows // 2), pl.ds(rows // 2, rows // 2)
    half = size // 2
    sources, targets = [], []
    part = w_hbm[0].shape[2]
    for i, ref in enumerate(w_hbm):
        base = part * (2 * (i // 2) + (z + i) % 2)
        for p in range(3):
            for kind in range(2):
                sources.append(ref.at[p, kind])
                targets.append(w_vm.at[p, pl.ds(base, part), pl.ds(kind * size, size)])
    loads = [pltpu.make_async_copy(src, dst, wsem.at[i]) for i, (src, dst) in enumerate(zip(sources, targets))]

    def vis_loads(s):
        spot = s % 2
        return [pltpu.make_async_copy(src.at[s], vis_vm.at[spot, i], vsem.at[spot, i]) for i, src in enumerate((own_hbm, par_hbm))]

    def kv_load(s):
        return pltpu.make_async_copy(kv_hbm.at[s], kv_vm.at[s % 2], kv_sem.at[s % 2])

    for ld in vis_loads(0) + [kv_load(0)]:
        ld.start()
    for ld in loads:
        ld.start()

    def near(ref, s, p):
        return ref.at[s, (1 - y) if p // 2 else y, (1 - x) if p % 2 else x]

    def ends(flow, s):
        own, sx, sy, sd = q_all.at[s, y, x], q_all.at[s, y, 1 - x], q_all.at[s, 1 - y, x], q_all.at[s, 1 - y, 1 - x]
        if flow == Q_X:
            return own, own, px, sx
        if flow == Q_Y:
            return own, own, py, sy
        if flow == Q_YF:
            return sx.at[top], sx.at[top], py, sd.at[top]
        if flow == Q_XF:
            return sy.at[low], sy.at[low], px, sd.at[low]
        if flow == O_X1:
            return ob_l.at[s, :, 1 - x], rec_x1.at[s], px, rec_x1.at[s]
        if flow == O_Y1:
            return ob_h.at[s, 1 - y], rec_y1.at[s], py, rec_y1.at[s]
        if flow == O_Y2:
            return two_l.at[s, 1 - y], rec_y2.at[s], py, rec_y2.at[s]
        return two_h.at[s, 1 - x], rec_x2.at[s], px, rec_x2.at[s]

    def descr(flow, s, incoming):
        src, dst, who, landing = ends(flow, s)
        return pltpu.make_async_remote_copy(src_ref=src, dst_ref=landing if incoming else dst, send_sem=send.at[flow, s], recv_sem=recv.at[flow, s], device_id={'tp': who}, device_id_type=MESH)

    def start(flow, s):
        descr(flow, s, False).start()

    def got(flow, s):
        descr(flow, s, True).wait_recv()

    barrier = pltpu.get_barrier_semaphore()
    for who in (px, py):
        pl.semaphore_signal(barrier, inc=1, device_id={'tp': who}, device_id_type=MESH)
    pl.semaphore_wait(barrier, 2)

    def stat_block(top_row, sum_row):
        return jnp.concatenate([top_row, sum_row] + [top_row] * (STAT - 2), axis=0)

    def merged(a, b):
        max_a, max_b = a[half:half + 1], b[half:half + 1]
        peak = jnp.maximum(max_a, max_b)
        fac_a, fac_b = jnp.exp(max_a - peak), jnp.exp(max_b - peak)
        total = a[half + 1:half + 2] * fac_a + b[half + 1:half + 2] * fac_b
        return a[:half] * fac_a + b[:half] * fac_b, peak, total

    def st_a(s):
        q_all[s, y, x] = q_ref[s]
        start(Q_X, s)
        start(Q_Y, s)

    def st_b(s):
        got(Q_X, s)
        start(Q_YF, s)
        got(Q_Y, s)
        start(Q_XF, s)

    def st_c(s):
        got(Q_YF, s)
        got(Q_XF, s)
        seen = seen_ref[s] > 0
        spot = s % 2
        for p in range(4):
            cols = pl.ds((p - 1) * size, size)
            keys = k_vm[spot, :, cols] if p else kv_vm[spot, :, pl.ds(0, size)]
            vals = v_vm[spot, :, cols] if p else kv_vm[spot, :, pl.ds(size, size)]
            scores = lax.dot_general(keys, near(q_all, s, p)[...], (((1,), (1,)), ((), ())), preferred_element_type=jnp.float32)
            peak = jnp.max(scores, axis=0, keepdims=True)
            weights = jnp.exp(scores - peak)
            total = jnp.sum(weights, axis=0, keepdims=True)
            context = lax.dot_general(vals, weights.astype(jnp.bfloat16), (((0,), (0,)), ((), ())), preferred_element_type=jnp.float32)
            stats = stat_block(jnp.where(seen, peak, MASK_VALUE), total)
            for ref, part in ((ob_l, context[:half]), (ob_h, context[half:])):
                near(ref, s, p)[:half] = part
                near(ref, s, p)[half:] = stats
        start(O_X1, s)
        start(O_Y1, s)

    def st_d(s):
        got(O_X1, s)
        for q in range(2):
            body, peak, total = merged(ob_l[s, q, x], rec_x1[s, q])
            two_l[s, q, :half] = body
            two_l[s, q, half:] = stat_block(peak, total)
        start(O_Y2, s)
        got(O_Y1, s)
        for q in range(2):
            body, peak, total = merged(ob_h[s, y, q], rec_y1[s, q])
            two_h[s, q, :half] = body
            two_h[s, q, half:] = stat_block(peak, total)
        start(O_X2, s)

    def st_e(s):
        got(O_Y2, s)
        got(O_X2, s)
        parts = []
        for mine, other in ((two_l[s, y], rec_y2[s]), (two_h[s, x], rec_x2[s])):
            body, _, total = merged(mine, other)
            parts.append(body / total)
        whole = jnp.concatenate(parts, axis=0).T.astype(jnp.bfloat16)
        reps = rows // ctx.shape[1]
        for r in range(reps):
            ctx[s, :, r * size:(r + 1) * size] = whole[r * ctx.shape[1]:(r + 1) * ctx.shape[1]]

    def st_j(s):
        @pl.when(s == 0)
        def _():
            for ld in loads:
                ld.wait()

        @pl.when(s + 1 < samples)
        def _():
            for ld in vis_loads(s + 1) + [kv_load(s + 1)]:
                ld.start()
        for ld in vis_loads(s) + [kv_load(s)]:
            ld.wait()
        spot = s % 2
        rows_in = vis_vm[spot].reshape(2 * vis_rows, -1)
        for p in range(3):
            cols = pl.ds(p * size, size)
            keys = jnp.dot(rows_in, w_vm[p, :, pl.ds(0, size)], preferred_element_type=jnp.float32)
            mean_sq = jnp.mean(keys * keys, axis=-1, keepdims=True)
            k_vm[spot, :, cols] = (keys * lax.rsqrt(mean_sq + NORM_EPS) * gain_ref[1:2].astype(jnp.float32)).astype(jnp.bfloat16)
            v_vm[spot, :, cols] = jnp.dot(rows_in, w_vm[p, :, pl.ds(size, size)], preferred_element_type=jnp.float32).astype(jnp.bfloat16)

    stages = [(st_d, 2), (st_e, 3), (st_c, 1), (st_b, 0), (st_j, 0)]

    def step(t, carry):
        for stage, lag in stages:
            s = t - lag

            @pl.when((s >= 0) & (s < samples))
            def _(stage=stage, s=s):
                stage(s)
        return carry

    def first(s, carry):
        st_a(s)
        return carry

    lax.fori_loop(0, samples, first, 0)
    lax.fori_loop(0, samples + 3, step, 0)

    def drain(s, carry):
        for flow in range(8):
            descr(flow, s, False).wait_send()
        return carry

    lax.fori_loop(0, samples, drain, 0)


def cross(cid, queries, seen, gain, own, partner, kv_own, weights, tokens):
    samples, rows, size = queries.shape
    vis_rows, dim = own.shape[1:]
    f32, bf16 = jnp.float32, jnp.bfloat16
    half = size // 2
    vmem = pl.BlockSpec(memory_space=pltpu.VMEM)
    hbm = pl.BlockSpec(memory_space=pl.ANY)
    wide = pltpu.VMEM((samples, 2, half + STAT, rows), f32)
    one = pltpu.VMEM((samples, half + STAT, rows), f32)
    both = pltpu.VMEM((samples, *PLANE, half + STAT, rows), f32)
    heads = pltpu.VMEM((2, 2 * vis_rows, 3 * size), bf16)
    return pl.pallas_call(
        functools.partial(cross_kernel, samples, len(weights)),
        out_shape=jax.ShapeDtypeStruct((samples, tokens, rows // tokens * size), bf16),
        in_specs=[vmem, vmem, vmem] + [hbm] * (3 + len(weights)), out_specs=vmem,
        scratch_shapes=[
            pltpu.VMEM((samples, *PLANE, rows, size), bf16), pltpu.VMEM((3, dim, 2 * size), bf16),
            pltpu.VMEM((2, 2, vis_rows, dim), bf16), pltpu.VMEM((2, 2 * vis_rows, 2 * size), bf16), heads, heads,
            both, both, wide, wide, wide, wide, one, one,
            pltpu.SemaphoreType.DMA((8, samples)), pltpu.SemaphoreType.DMA((8, samples)),
            pltpu.SemaphoreType.DMA((24,)), pltpu.SemaphoreType.DMA((2, 2)), pltpu.SemaphoreType.DMA((2,))],
        name=f'cross_{cid}',
        cost_estimate=pl.CostEstimate(flops=8 * 10 ** 10, bytes_accessed=10 ** 7, transcendentals=0),
        compiler_params=pltpu.CompilerParams(collective_id=cid, has_side_effects=True, vmem_limit_bytes=60 * 2 ** 20),
    )(queries, seen, gain, own, partner, kv_own, *weights)


def solution(mesh):
    act_spec = P('dp', 'tp', None)
    col_spec = P(None, 'tp')
    row_spec = P('tp', None)
    layer_a = (P(), col_spec, col_spec, col_spec, row_spec, P(), col_spec, col_spec, row_spec)
    layer_b = (P(), col_spec, P(), col_spec, col_spec, P(), row_spec, P(), col_spec, col_spec, row_spec, P())
    in_specs = (act_spec, act_spec, P('dp', 'tp'), act_spec) + layer_a + layer_b

    def body(hidden, vision, positions, tile_mask, ln1_a, wq_a, wk_a, wv_a, wo_a, ln2_a, wg_a, wu_a, wd_a, ln1_b, wq_b, q_norm, wk_b, wv_b, k_norm, wo_b, ln2_b, wg_b, wu_b, wd_b, xgates):
        me = lax.axis_index('tp')
        head_dim = q_norm.shape[0]
        samples, rows, model_dim = hidden.shape
        tokens = rows * 8
        tiles = tile_mask.shape[2]
        kv_local = wk_a.shape[1] // head_dim
        rep_heads = wq_a.shape[1] // head_dim // kv_local

        gains = jnp.stack([g.astype(jnp.float32) for g in (ln1_a, ln2_a, ln1_b, ln2_b)])
        head_gains = jnp.stack([q_norm.astype(jnp.float32), k_norm.astype(jnp.float32)])
        vis_partner = lax.ppermute(vision, 'tp', [(i, i ^ 1) for i in range(8)])

        small = jnp.concatenate([positions.reshape(-1), tile_mask.reshape(-1)])
        aux = jnp.pad(small, (0, 1024 - small.shape[0])).reshape(8, 128)
        proj, aux_all, near_one = fused(1, hidden, gain=gains, gain_row=0, w_post=(wq_a, wk_a, wv_a), aux=aux, mine=(wk_b, wv_b), near_part=0)
        aux_all = aux_all.reshape(8, 1024)
        pos_all = aux_all[:, :samples * rows].reshape(8, samples, rows).transpose(1, 0, 2).reshape(samples, tokens)
        mask_all = aux_all[:, samples * rows:samples * rows * (1 + tiles)].reshape(8, samples, rows, tiles).transpose(1, 0, 2, 3).reshape(samples, tokens, tiles)

        angles = pos_all.astype(jnp.float32)[..., None] * rope_table(head_dim)
        rope = (jnp.cos(angles), jnp.sin(angles))
        h_one, act, near_two, far_one = fused(2, hidden, lhs=proj, w_pre=wo_a, rope=rope, gain=gains, gain_row=1, w_post=(wg_a, wu_a), mode='swiglu', mine=(wk_b, wv_b), near_part=1, far_src=near_one)
        h_two, queries, kv_own, far_two = fused(3, h_one, lhs=act, w_pre=wd_a, gain=gains, gain_row=2, w_post=(wq_b,), mode='queries', q_gain=head_gains, far_src=near_two, kv=(vision, vis_partner, wk_b, wv_b))
        weights = (near_one, far_one, near_two, far_two)
        seen = jnp.tile(lax.dynamic_index_in_dim(mask_all, me // 2, axis=2, keepdims=False)[:, None, :], (1, 1, rep_heads))
        context = cross(6, queries, seen, head_gains, vision, vis_partner, kv_own, weights, tokens)
        h_three, act = fused(4, h_two, lhs=context, w_pre=wo_b, gate=(tile_mask, xgates, 0), gain=gains, gain_row=3, w_post=(wg_b, wu_b), mode='swiglu')
        return fused(5, h_three, lhs=act, w_pre=wd_b, gate=(tile_mask, xgates, 1))[0]

    return jax.shard_map(body, mesh=mesh, in_specs=in_specs, out_specs=act_spec, check_vma=False)
```
